256 devices in a mesh: grp: 4 (over y), slab: 64 (over z, x, core).
Axes of the slice: x: 4, y: 4, z: 8, core: 2. Of those that a mesh axis runs over, the one named last changes fastest.
Arguments:
- pressure_pair: float32 [2, 1024, 256], P(None, ('grp', 'slab')), may hold values from -6 to 6
- normals: float32 [3, 1024, 256], P(None, ('grp', 'slab')), may hold values from -6 to 6
- mesh_disp: float32 [3, 1024, 128, 256], P(None, ('grp', 'slab')), may hold values from -6 to 6
- kappa: float32 [1024, 128, 256], P(('grp', 'slab')), may hold values from 1 to 10
- face_owner: int32 [262144, 1], P(('grp', 'slab')), may hold values from 0 to 63; in each aligned block of 1024 rows (0 to 1023, 1024 to 2047, ...) at most 32 rows name the same one
- face_node: int32 [262144], P(('grp', 'slab')), may hold values from 0 to 1023
- stiffness: float32 [24, 24, 262144], P(None, None, ('grp', 'slab')), may hold values from -1 to 3, as said below
- shell_conn: int32 [4, 262144], P(None, ('grp', 'slab')), may hold values from 0 to 1151
- precond: float32 [6, 262144], P(None, ('grp', 'slab')), may hold values from 0.1 to 0.3
Outputs:
- mesh_out: float32 [3, 1024, 128, 256], P(None, ('grp', 'slab'))
- shell_disp: float32 [6, 262144], P(None, ('grp', 'slab'))
The draws below stay inside these ranges and needn't reach their ends.
Inputs may be any that keep to these rules, and one draw needn't show every extreme that they name: `face_owner`: within the 1024 faces of one device's block no owner is named by more than 32 faces, a bound that some block reaches. `stiffness`: each element's block is symmetric with diagonal entries between 2 and 3.
All inputs are finite; a program needn't handle non-finite values.
Results may differ from the reference program's by a relative error of at most 0.00011.
Values sent between devices are 32-bit elements; how exact they have to be, the bound alone decides.
No kernel may reach another device: no remote copies, remote signals or barrier semaphores. Data moves between devices by JAX's collectives and lax.ppermute only.
A program may use at most 64 MiB of HBM per device.

```python
import math
import jax
import jax.numpy as jnp
import numpy as np
from jax import lax

CZ = 4
NY = 128
NX = 256
E_DEV = 1024
NB = 128
NN_DEV = 1024
CAP = 32
NZ = 1024
N_GRP = 4
N_SLAB = 64


def draw_stiffness(key, part):
    total = N_GRP * N_SLAB * E_DEV
    key_off = jax.random.fold_in(key, 11)
    key_diag = jax.random.fold_in(key, 12)
    raw = jnp.clip(0.08 * jax.random.normal(key_off, (24, 24, total), jnp.float32), -0.4, 0.4)
    symmetric = (raw + jnp.transpose(raw, (1, 0, 2))) * 0.7071
    diagonal = jax.random.uniform(key_diag, (24, total), jnp.float32, 2.0, 3.0)
    eye = jnp.eye(24, dtype=jnp.float32)[:, :, None]
    return symmetric * (1.0 - eye) + eye * diagonal[None, :, :]


def plant(array, rng, low, top_value):
    longest = array.shape.index(max(array.shape))
    spots = []
    for shift in (0, 1):
        where = [jax.random.randint(jax.random.fold_in(rng, axis), (), 0, length) for axis, length in enumerate(array.shape)]
        where[longest] = (where[longest] + shift) % array.shape[longest]
        spots.append(tuple(where))
    return array.at[spots[0]].set(low).at[spots[1]].set(top_value)


def levels(stream_key, shape, cuts, low, top_value):
    def one(axis_at, parts):
        heights = jax.random.uniform(jax.random.fold_in(jax.random.fold_in(stream_key, 6), axis_at), (parts,), jnp.float32, low / len(cuts), top_value / len(cuts))
        return jnp.repeat(jnp.exp(heights), shape[axis_at] // parts).reshape((-1,) + (1,) * (len(shape) - axis_at - 1))

    gain = one(*cuts[0])
    for cut in cuts[1:]:
        gain = gain * one(*cut)
    return gain


def deal_out(key, own, number, rows, count, top, most, slope):
    ranking = jax.random.permutation(key, count)
    heavy_load, ordinary = shares(count, rows * top, most, slope, True), shares(count, rows * top, most, slope, False)
    places = jnp.arange(count)

    def named(lengths, rotation):
        used = int((lengths > 0).sum())
        fixed = max(1, used // 4)
        moved = fixed + (places - fixed + rotation * (used - fixed)) % max(1, count - fixed)
        return jnp.zeros((count,), jnp.int32).at[ranking[jnp.where(places < fixed, places, moved)]].set(jnp.asarray(lengths, jnp.int32))

    lengths = jnp.where(number % 4 == 0, named(heavy_load, number // 4), named(ordinary, number - number // 4 - 1))
    mixed = jax.random.permutation(jax.random.fold_in(own, 3), count)
    giver, taker = mixed[0:count // 2 * 2:2], mixed[1:count // 2 * 2:2]
    slack = jnp.minimum(lengths[giver] - 1, most - lengths[taker]) // 2
    slack = jnp.where((giver == ranking[0]) | (taker == ranking[0]) | (lengths[taker] == 0), 0, jnp.maximum(slack, 0))
    moved = jax.random.randint(jax.random.fold_in(own, 4), (count // 2,), 0, 1 << 20) % (slack + 1)
    lengths = lengths.at[giver].add(-moved).at[taker].add(moved)
    labels = jnp.searchsorted(jnp.cumsum(lengths), jnp.arange(rows * top), side="right").astype(jnp.int32)
    grid = labels.reshape(top, rows).T
    grid = grid[jax.random.permutation(jax.random.fold_in(own, 1), rows)]
    rotation = jax.random.randint(jax.random.fold_in(own, 2), (rows, 1), 0, top)
    return jnp.take_along_axis(grid, (jnp.arange(top)[None, :] + rotation) % top, axis=1)


def shares(number_of, total, limit, lean, full):
    weights = [(1 << 20) // math.isqrt(rank ** lean) + 1 for rank in range(1, number_of + 1)]
    largest = limit if full else min(limit, max(-(-total // number_of), total * weights[0] // sum(weights)))
    least = 1 if total - largest >= number_of - 1 else 0
    counts, surplus = [largest] + [least] * (number_of - 1), total - largest - least * (number_of - 1)
    while surplus > 0:
        free = [i for i in range(1, number_of) if counts[i] < largest] or [i for i in range(1, number_of) if counts[i] < limit]
        mass, budget = sum([weights[i] for i in free]), surplus
        for i in free:
            addition = min(limit - counts[i], max(1, budget * weights[i] // mass), surplus)
            counts[i] = counts[i] + addition
            surplus = surplus - addition
    return np.array(counts)


def noise(own_key, extent, spread, most, cuts=(), kind=jnp.bfloat16):
    drawn = spread * jax.random.normal(own_key, extent, jnp.float32)
    if cuts:
        drawn = drawn * levels(own_key, extent, cuts, -0.22, 0.18)
    return jnp.clip(drawn, -most, most).astype(kind)


def setup_inputs(seed: int = 0) -> dict:
    key_list = jax.random.split(jax.random.key(seed), 10)
    pressure_pair = noise(key_list[0], (2, NZ, NX), 1.0, 6.0, ((1, 256),), jnp.float32)
    normals = noise(key_list[1], (3, NZ, NX), 1.0, 6.0, ((1, 256),), jnp.float32)
    mesh_disp = noise(key_list[2], (3, NZ, NY, NX), 1.0, 6.0, ((1, 256),), jnp.float32)
    kappa = jnp.clip(jnp.exp(math.log(10.0) - 2.3025851 * jax.random.uniform(key_list[3], (NZ, NY, NX), jnp.float32) ** levels(key_list[3], (NZ, NY, NX), ((0, 256),), -0.2, 0.2)), 1.0, 10.0)
    face_owner_keys = jax.random.split(jax.random.fold_in(key_list[4], 1), (NZ * NX) // (CZ * NX))
    face_owner_turns = jax.random.permutation(jax.random.fold_in(key_list[4], 3), (NZ * NX) // (CZ * NX))
    face_owner = jax.vmap(lambda own, number: deal_out(jax.random.fold_in(key_list[4], 2), own, number, CZ * NX, N_SLAB, 1, CAP, 2))(face_owner_keys, face_owner_turns).reshape((NZ * NX, 1))
    face_node = plant(jax.random.randint(key_list[5], (NZ * NX,), 0, NN_DEV), jax.random.fold_in(key_list[5], 1), 0, NN_DEV - 1).astype(jnp.int32)
    stiffness = draw_stiffness(jax.random.fold_in(key_list[9], 71), 0)
    shell_conn = plant(jax.random.randint(key_list[7], (4, N_GRP * N_SLAB * E_DEV), 0, NN_DEV + NB), jax.random.fold_in(key_list[7], 1), 0, (NN_DEV + NB) - 1).astype(jnp.int32)
    precond = jnp.clip(jnp.exp(math.log(0.3) - 1.0986123 * jax.random.uniform(key_list[8], (6, N_GRP * N_SLAB * NN_DEV), jnp.float32) ** levels(key_list[8], (6, N_GRP * N_SLAB * NN_DEV), ((1, 256),), -0.2, 0.2)), 0.1, 0.3)
    return {"pressure_pair": pressure_pair, "normals": normals, "mesh_disp": mesh_disp, "kappa": kappa, "face_owner": face_owner, "face_node": face_node, "stiffness": stiffness, "shell_conn": shell_conn, "precond": precond}


def relax(field_ext, kappa_ext, level):
    center_k = kappa_ext[1:-1]
    padded_k = jnp.pad(center_k, ((0, 0), (1, 1), (1, 1)), mode="edge")
    padded_m = jnp.pad(field_ext[:, 1:-1], ((0, 0), (0, 0), (1, 1), (1, 1)))
    pairs = [
        (kappa_ext[2:], field_ext[:, 2:]),
        (kappa_ext[:-2], field_ext[:, :-2]),
        (padded_k[:, 2:, 1:-1], padded_m[:, :, 2:, 1:-1]),
        (padded_k[:, :-2, 1:-1], padded_m[:, :, :-2, 1:-1]),
        (padded_k[:, 1:-1, 2:], padded_m[:, :, 1:-1, 2:]),
        (padded_k[:, 1:-1, :-2], padded_m[:, :, 1:-1, :-2]),
    ]
    weighted = jnp.zeros(field_ext[:, 1:-1].shape, jnp.float32)
    weight_sum = jnp.zeros(center_k.shape, jnp.float32)
    for near_k, near_m in pairs:
        weight = 0.5 * (center_k + near_k)
        weighted = weighted + weight[None] * near_m
        weight_sum = weight_sum + weight
    relaxed = weighted / weight_sum[None]
    return relaxed.at[:, :, level, :].set(field_ext[:, 1:-1, level, :])


def reference(pressure_pair, normals, mesh_disp, kappa, face_owner, face_node, stiffness, shell_conn, precond):
    fluid_rows = NZ
    face_total = fluid_rows * NX
    node_total = N_SLAB * NN_DEV
    shell_elems = N_SLAB * E_DEV
    level = NY // 2
    traction = ((pressure_pair[0] - pressure_pair[1])[None] * normals).reshape(3, face_total)
    owners = face_owner[:, 0]
    targets = (owners * NN_DEV + face_node).astype(jnp.int32)
    forces = jnp.zeros((3, node_total), jnp.float32).at[:, targets].add(traction)
    loading = jnp.concatenate([forces, jnp.zeros((3, node_total), jnp.float32)], 0)
    elem_start = stiffness.shape[2] - shell_elems
    element_k = stiffness[:, :, elem_start:]
    connect = shell_conn[:, elem_start:]
    partition = (jnp.arange(shell_elems, dtype=jnp.int32) // E_DEV).astype(jnp.int32)
    global_node = (partition[None] * NN_DEV + connect).astype(jnp.int32)
    inside = global_node < node_total
    safe_node = jnp.where(inside, global_node, 0).astype(jnp.int32)
    drop_node = jnp.where(inside, global_node, node_total).astype(jnp.int32)
    inside_f = inside.astype(jnp.float32)
    scaling = precond[:, precond.shape[1] - node_total:]

    def apply(values):
        gathered = jnp.stack([values[:, safe_node[a]] * inside_f[a][None] for a in range(4)]).reshape(24, shell_elems)
        element_force = jnp.einsum("ije,je->ie", element_k, gathered, precision=lax.Precision.HIGHEST)
        nodal = jnp.zeros((6, node_total + 1), jnp.float32)
        for a in range(4):
            nodal = nodal.at[:, drop_node[a]].add(element_force[6 * a:6 * a + 6])
        return nodal[:, :node_total]

    first_step = scaling * loading
    second_step = first_step + scaling * (loading - apply(first_step))
    third_step = second_step + scaling * (loading - apply(second_step))
    shell_disp = jnp.concatenate([jnp.zeros((6, precond.shape[1] - node_total), jnp.float32), third_step], 1)
    face_motion = third_step[:3][:, targets].reshape(3, fluid_rows, NX)
    field = mesh_disp.at[:, :, level, :].set(face_motion)
    kappa_ext = jnp.pad(kappa, ((1, 1), (0, 0), (0, 0)), mode="edge")
    for sweep in range(2):
        field_ext = jnp.pad(field, ((0, 0), (1, 1), (0, 0), (0, 0)))
        field = relax(field_ext, kappa_ext, level)
    return field, shell_disp
```

```python
import jax
import jax.numpy as jnp
from jax import lax
from jax.experimental import pallas as pl
from jax.experimental.pallas import tpu as pltpu
from jax.sharding import PartitionSpec as P

F32 = jnp.float32
BF16 = jnp.bfloat16
AXES = ("grp", "slab")
CAP = 32
NB = 128
NODES = 1024
EXT = NODES + NB
NBLK = EXT // 128
ELEMS = 1024
LOW = 56
VMEM = pl.BlockSpec(memory_space=pltpu.VMEM)
ANY = pl.BlockSpec(memory_space=pl.ANY)
PARAMS = pltpu.CompilerParams(vmem_limit_bytes=40 * 1024 * 1024)


def nn(a, b):
    return lax.dot_general(a, b, (((1,), (0,)), ((), ())), preferred_element_type=F32)


def nt(a, b):
    return lax.dot_general(a, b, (((1,), (1,)), ((), ())), preferred_element_type=F32)


def split(x):
    high = x.astype(BF16).astype(F32)
    return high, x - high


def iota(shape, dim):
    return lax.broadcasted_iota(jnp.int32, shape, dim)


def hot(mask):
    return jnp.where(mask, 1.0, 0.0).astype(F32)


def cat(parts, axis):
    return jnp.concatenate(parts, axis=axis)


def pack_kernel(slabs, pp, nm, own, nod, send, place):
    owners = own[...]
    nodes = nod[...].astype(F32)
    depth = pp.shape[1]

    def layer(a, z):
        return cat([a[2 * z : 2 * z + 1], a[2 * z + 1 : 2 * z + 2]], 1)

    ow = [layer(owners, z) for z in range(depth)]
    nd = [layer(nodes, z) for z in range(depth)]
    ids = iota((slabs, 256), 0)
    member = [hot(ow[z] == ids) for z in range(depth)]
    before = hot(iota((256, 256), 0) < iota((256, 256), 1)).astype(BF16)
    counts = nn(cat(member, 0).astype(BF16), before)
    offset = jnp.zeros((slabs, 1), F32)
    slot = iota((4 * CAP, 256), 0)
    rank_row = (slot // 4).astype(F32)
    comp = slot % 4
    words = []
    for z in range(depth):
        seen = counts[slabs * z : slabs * (z + 1)] + offset
        rank = jnp.sum(member[z] * seen, axis=0, keepdims=True)
        offset = offset + jnp.sum(member[z], axis=1, keepdims=True)
        place[z : z + 1] = ow[z].astype(F32) * CAP + rank
        jump = pp[0, z : z + 1] - pp[1, z : z + 1]
        t0, t1, t2 = [jump * nm[c, z : z + 1] for c in range(3)]
        value = jnp.where(comp == 0, t0, jnp.where(comp == 1, t1, jnp.where(comp == 2, t2, nd[z])))
        words.append(jnp.where(rank == rank_row, value, 0.0))
    place[depth:8] = jnp.zeros((8 - depth, 256), F32)
    high, low = split(cat(words, 1))
    members = cat(member, 1).astype(BF16)
    packed = nt(members, high.astype(BF16)) + nt(members, low.astype(BF16))
    ahead = cat([packed[1:], jnp.zeros((1, 4 * CAP), F32)], 0)
    first = send.shape[0] - 2 * slabs
    send[0:first] = jnp.zeros((first, 128), F32)
    send[pl.ds(first, slabs, stride=2), :] = packed
    send[pl.ds(first + 1, slabs, stride=2), :] = ahead


def connect(conn, table):
    c = conn[...]
    blocks = []
    for a in range(4):
        n = c[a : a + 1]
        blocks.append(n >> 7)
        table[:, a * ELEMS : (a + 1) * ELEMS] = hot(iota((128, ELEMS), 0) == (n & 127)).astype(BF16)
    return blocks


def stiff(values, blocks, stiffness, table, spread):
    high, low = split(values)
    parts = []
    for b in range(NBLK):
        lanes = slice(128 * b, 128 * b + 128)
        parts += [high[:, lanes], low[:, lanes]]
    stack = cat(parts, 0).astype(BF16)
    gathered = []
    for a in range(4):
        wide = nn(stack, table[:, a * ELEMS : (a + 1) * ELEMS])
        total = jnp.zeros((8, ELEMS), F32)
        for b in range(NBLK):
            row = wide[16 * b : 16 * b + 8] + wide[16 * b + 8 : 16 * b + 16]
            total = total + jnp.where(blocks[a] == b, row, 0.0)
        gathered.append(total)
    chunk = 256
    pieces = []
    for e in range(0, ELEMS, chunk):
        acc = jnp.zeros((24, chunk), F32)
        for a in range(4):
            for c in range(6):
                acc = acc + stiffness[a * 6 + c, :, e : e + chunk] * gathered[a][c : c + 1, e : e + chunk]
        pieces.append(acc)
    force = cat(pieces, 1)
    for a in range(4):
        part = cat([force[6 * a : 6 * a + 6], jnp.zeros((2, ELEMS), F32)], 0)
        both = cat(split(part), 0)
        for b in range(NBLK):
            spread[16 * b : 16 * b + 16, a * ELEMS : (a + 1) * ELEMS] = jnp.where(
                blocks[a] == b, both, 0.0
            ).astype(BF16)
    summed = nt(spread[...], table[...])
    return cat([summed[16 * b : 16 * b + 8] + summed[16 * b + 8 : 16 * b + 16] for b in range(NBLK)], 1)


def fold(tile):
    both = tile + pltpu.roll(tile, 4, 0)
    return jnp.where(iota(tile.shape, 0) < 3, both, 0.0)


def diagonal(precond, ghost):
    return cat([cat([precond[...], jnp.zeros((2, NODES), F32)], 0), ghost[...]], 1)


def load_kernel(recv, precond, ghost, conn, stiffness, load, first, partial, spill, edge,
                held, table, spread, slots, marks, sem):
    fetch = pltpu.make_async_copy(stiffness, held, sem)
    fetch.start()
    blocks = connect(conn, table)
    senders = recv.shape[0] // 2
    ids = iota((128, senders), 0).astype(F32)
    sums = []
    for which in range(2):
        data = recv[pl.ds(which, senders, stride=2), :].T
        high, low = split(data)
        for r in range(CAP):
            lanes = slice(r * senders, (r + 1) * senders)
            node = data[4 * r + 3 : 4 * r + 4]
            both = cat([high[4 * r : 4 * r + 4], low[4 * r : 4 * r + 4]], 0)
            if which == 0:
                block = jnp.floor(node * (1.0 / 128.0))
                node = node - 128.0 * block
                for b in range(0, 8, 2):
                    slots[8 * b : 8 * b + 16, lanes] = cat(
                        [jnp.where(block == b + k, both, 0.0) for k in range(2)], 0
                    ).astype(BF16)
            else:
                slots[0:16, lanes] = cat([both, jnp.zeros_like(both)], 0).astype(BF16)
            marks[:, lanes] = hot(ids == node).astype(BF16)
        if which == 0:
            found = nt(slots[...], marks[...])
            sums += [fold(found[8 * b : 8 * b + 8]) for b in range(8)]
        else:
            sums += [fold(nt(slots[0:16], marks[...])[0:8])]
    loading = cat(sums, 1)
    start = diagonal(precond, ghost) * loading
    load[...] = loading
    first[...] = start
    fetch.wait()
    result = stiff(start, blocks, held, table, spread)
    partial[...] = result
    spill[...] = result[:, NODES:]
    edge[...] = result[:, :NB]


def step_kernel(load, first, partial, from_low, from_high, precond, ghost, conn, stiffness, second, spill,
                held, table, spread, sem):
    fetch = pltpu.make_async_copy(stiffness, held, sem)
    fetch.start()
    blocks = connect(conn, table)
    scale = diagonal(precond, ghost)
    loading = load[...]
    extra = cat([from_low[...], jnp.zeros((8, NODES - NB), F32), from_high[...]], 1)
    values = first[...] + scale * (loading - (partial[...] + extra))
    fetch.wait()
    result = stiff(values, blocks, held, table, spread)
    own = values + scale * (loading - result)
    second[...] = own[:, :NODES]
    spill[...] = result[:, NODES:]


def reply_kernel(second, precond, from_low, recv, send, shell):
    shift = precond[:, :NB] * from_low[0:6]
    near = second[:, :NB] - cat([shift, jnp.zeros((2, NB), F32)], 0)
    values = cat([near, second[:, NB:]], 1)
    shell[...] = values[0:6]
    high, low = split(values)
    senders = recv.shape[0] // 2
    stack = cat(
        [
            part[0:4, 128 * b : 128 * b + 128]
            for b in range(NODES // 128)
            for part in (high, low)
        ],
        0,
    ).astype(BF16)
    data = recv[pl.ds(0, senders, stride=2), :].T
    ids = iota((128, senders), 0).astype(F32)
    upper = iota((8, senders), 0) < 4
    tiles = []
    for t in range(CAP // 2):
        pair = []
        for r in (2 * t, 2 * t + 1):
            node = data[4 * r + 3 : 4 * r + 4]
            block = jnp.floor(node * (1.0 / 128.0))
            wide = nn(stack, hot(ids == node - 128.0 * block).astype(BF16))
            total = jnp.zeros((8, senders), F32)
            for b in range(NODES // 128):
                total = total + jnp.where(block == b, wide[8 * b : 8 * b + 8], 0.0)
            pair.append(total + pltpu.roll(total, 4, 0))
        tiles.append(jnp.where(upper, pair[0], pair[1]))
    answer = cat(tiles, 0).T
    send[pl.ds(0, senders, stride=3), :] = cat([answer[senders - 1 :], answer[: senders - 1]], 0)
    send[pl.ds(1, senders, stride=3), :] = answer
    send[pl.ds(2, senders, stride=3), :] = cat([answer[1:], answer[:1]], 0)


def sweep_kernel(field, kappa, low_field, low_kappa, high_field, high_kappa, out, mid, factors,
                 kext, fext, mext, done, sems, out_sem):
    depth = field.shape[1]
    rows, cols = field.shape[2:]
    level = rows // 2
    flat = lax.axis_index("grp") * lax.axis_size("slab") + lax.axis_index("slab")
    last = lax.axis_size("grp") * lax.axis_size("slab") - 1
    copies = [
        pltpu.make_async_copy(src, dst, sems.at[i])
        for i, (src, dst) in enumerate(
            [
                (low_kappa, kext.at[0:2]),
                (kappa, kext.at[2 : depth + 2]),
                (high_kappa, kext.at[depth + 2 : depth + 4]),
                (low_field, fext.at[:, 0:2]),
                (field, fext.at[:, 2 : depth + 2]),
                (high_field, fext.at[:, depth + 2 : depth + 4]),
            ]
        )
    ]
    for copy in copies:
        copy.start()
    for copy in copies:
        copy.wait()

    @pl.when(flat == 0)
    def _():
        kext[1] = kext[2]

    @pl.when(flat == last)
    def _():
        kext[depth + 2] = kext[depth + 1]

    row = iota((rows, cols), 0)
    col = iota((rows, cols), 1)

    def weights(l):
        k = kext[l]
        down = k + jnp.where(row == 0, k, pltpu.roll(k, 1, 0))
        up = k + jnp.where(row == rows - 1, k, pltpu.roll(k, rows - 1, 0))
        left = k + jnp.where(col == 0, k, pltpu.roll(k, 1, 1))
        right = k + jnp.where(col == cols - 1, k, pltpu.roll(k, cols - 1, 1))
        back = k + kext[l - 1]
        front = k + kext[l + 1]
        inverse = 1.0 / (down + up + left + right + back + front)
        return (
            jnp.where(row == 0, 0.0, down) * inverse,
            jnp.where(row == rows - 1, 0.0, up) * inverse,
            jnp.where(col == 0, 0.0, left) * inverse,
            jnp.where(col == cols - 1, 0.0, right) * inverse,
            back * inverse,
            front * inverse,
        )

    def blend(w, here, before, after):
        down, up, left, right, back, front = w
        total = down * pltpu.roll(here, 1, 0) + up * pltpu.roll(here, rows - 1, 0)
        total = total + left * pltpu.roll(here, 1, 1) + right * pltpu.roll(here, cols - 1, 1)
        total = total + back * before + front * after
        return jnp.where(row == level, 0.0, total)

    fext[:, :, level : level + 1, :] = jnp.zeros((3, depth + 4, 1, cols), F32)

    def first_sweep(i, carry):
        l = i + 1
        w = weights(l)
        down, up, left, right, back, front = w
        outside = jnp.logical_or(
            jnp.logical_and(flat == 0, i == 0), jnp.logical_and(flat == last, i == depth + 1)
        )
        keep = jnp.where(outside, 0.0, 1.0)
        a, b = level - 1, level - 2
        c, d = level + 1, level + 2
        picked = [
            up[a : a + 1] * keep, back[a : a + 1], front[a : a + 1], left[a : a + 1], right[a : a + 1],
            up[b : b + 1],
            down[c : c + 1] * keep, back[c : c + 1], front[c : c + 1], left[c : c + 1], right[c : c + 1],
            down[d : d + 1],
        ]
        factors[i] = cat(picked + [jnp.zeros((4, cols), F32)], 0)
        for comp in range(3):
            mext[comp, i] = blend(w, fext[comp, l], fext[comp, l - 1], fext[comp, l + 1]) * keep
        return carry

    lax.fori_loop(0, depth + 2, first_sweep, 0)

    def second_sweep(z, carry):
        w = weights(z + 2)
        for comp in range(3):
            value = blend(w, mext[comp, z + 1], mext[comp, z], mext[comp, z + 2])
            done[comp, z] = value
            mid[comp, z] = value[LOW : LOW + 16]
        return carry

    lax.fori_loop(0, depth, second_sweep, 0)
    store = pltpu.make_async_copy(done, out, out_sem)
    store.start()
    store.wait()


def finish_kernel(slabs, recv, place, low_place, high_place, factors, mid, base, out, rows16, sem):
    depth = mid.shape[1]
    cols = mid.shape[3]
    first = recv.shape[0] - 3 * slabs
    slot = iota((4 * CAP, cols), 0)
    rank_row = (slot // 4).astype(F32)
    ids = iota((slabs, cols), 0).astype(F32)
    views = []
    for j in range(3):
        part = recv[pl.ds(first + j, slabs, stride=3), :]
        views.append(cat(split(part), 0).T.astype(BF16))
    sources = [(0, low_place[0:1])] + [(1, place[z : z + 1]) for z in range(depth)] + [(2, high_place[0:1])]
    motion = []
    for j, where in sources:
        owner = jnp.floor(where * (1.0 / CAP))
        rank = where - CAP * owner
        member = hot(owner == ids).astype(BF16)
        wide = nn(views[j], cat([member, member], 0))
        kept = jnp.where(rank == rank_row, wide, 0.0)
        total = kept[0:8]
        for t in range(1, 4 * CAP // 8):
            total = total + kept[8 * t : 8 * t + 8]
        motion.append(total + pltpu.roll(total, 4, 0))
    f = factors
    near = [[f[i, 6 * s : 6 * s + 1] * motion[i] for i in range(depth + 2)] for s in range(2)]
    for z in range(depth):
        i = z + 1
        added = []
        for s in range(2):
            o = 6 * s
            d = near[s]
            side = (
                f[i, o + 1 : o + 2] * d[i - 1]
                + f[i, o + 2 : o + 3] * d[i + 1]
                + f[i, o + 3 : o + 4] * pltpu.roll(d[i], 1, 1)
                + f[i, o + 4 : o + 5] * pltpu.roll(d[i], cols - 1, 1)
                + d[i]
            )
            added.append((side, f[i, o + 5 : o + 6] * d[i]))
        (below, below2), (above, above2) = added
        for comp in range(3):
            k = slice(comp, comp + 1)
            change = cat(
                [jnp.zeros((6, cols), F32), below2[k], below[k], motion[i][k], above[k], above2[k],
                 jnp.zeros((5, cols), F32)], 0
            )
            rows16[comp, z] = mid[comp, z] + change
    store = pltpu.make_async_copy(rows16, out.at[:, :, LOW : LOW + 16, :], sem)
    store.start()
    store.wait()


def shape(*dims):
    return jax.ShapeDtypeStruct(dims, F32)


def call(kernel, ins, outs, scratch=(), aliases=None, any_ins=(), any_outs=(), name=None):
    return pl.pallas_call(
        kernel,
        out_shape=outs,
        in_specs=[ANY if i in any_ins else VMEM for i in range(len(ins))],
        out_specs=[ANY if i in any_outs else VMEM for i in range(len(outs))],
        scratch_shapes=list(scratch),
        input_output_aliases=aliases or {},
        compiler_params=PARAMS,
        name=name,
    )(*ins)


def exchange(rows, per, count):
    flat = rows.reshape(count, 1, per * 128)
    return lax.all_to_all(flat, AXES, 0, 0, tiled=True).reshape(count * per, 128)


def on_device(
    pressure_pair, normals, mesh_disp, kappa, face_owner, face_node, stiffness, shell_conn, precond
):
    groups = lax.axis_size("grp")
    slabs = lax.axis_size("slab")
    count = groups * slabs
    depth, height, across = mesh_disp.shape[1:]
    up = [(i, i + 1) for i in range(count - 1)]
    down = [(b, a) for a, b in up]
    shell = count - slabs
    shell_up = [(shell + i, shell + i + 1) for i in range(slabs - 1)]
    shell_down = [(b, a) for a, b in shell_up]

    send, place = call(
        lambda *refs: pack_kernel(slabs, *refs),
        [pressure_pair, normals, face_owner.reshape(8, 128), face_node.reshape(8, 128)],
        [shape(2 * count, 128), shape(8, across)],
        name="pack",
    )
    ghost_own = jnp.pad(precond[:, :NB], ((0, 2), (0, 0)))
    small_down = jnp.concatenate([ghost_own, place[0:1].reshape(2, 128), jnp.zeros((6, 128), F32)], 0)
    small_up = place[depth - 1 : depth].reshape(2, 128)
    from_high = lax.ppermute(small_down, AXES, down)
    from_low = lax.ppermute(small_up, AXES, up)
    ghost = from_high[0:8]
    high_place = from_high[8:10].reshape(1, across)
    low_place = from_low.reshape(1, across)

    recv = exchange(send, 2, count)
    low_field = lax.ppermute(mesh_disp[:, depth - 2 :], AXES, up)
    high_field = lax.ppermute(mesh_disp[:, :2], AXES, down)
    low_kappa = lax.ppermute(kappa[depth - 2 :], AXES, up)
    high_kappa = lax.ppermute(kappa[:2], AXES, down)

    dense = [
        pltpu.VMEM((24, 24, ELEMS), F32),
        pltpu.VMEM((128, 4 * ELEMS), BF16),
        pltpu.VMEM((16 * NBLK, 4 * ELEMS), BF16),
    ]
    load, first, partial, spill, edge = call(
        load_kernel,
        [recv, precond, ghost, shell_conn, stiffness],
        [shape(8, EXT), shape(8, EXT), shape(8, EXT), shape(8, NB), shape(8, NB)],
        dense
        + [pltpu.VMEM((64, count * CAP), BF16), pltpu.VMEM((128, count * CAP), BF16), pltpu.SemaphoreType.DMA],
        any_ins=(4,),
        name="load",
    )
    spill_low = lax.ppermute(spill, AXES, shell_up)
    edge_high = lax.ppermute(edge, AXES, shell_down)
    second, spill = call(
        step_kernel,
        [load, first, partial, spill_low, edge_high, precond, ghost, shell_conn, stiffness],
        [shape(8, NODES), shape(8, NB)],
        dense + [pltpu.SemaphoreType.DMA],
        any_ins=(8,),
        name="step",
    )
    spill_low = lax.ppermute(spill, AXES, shell_up)
    send, shell_disp = call(
        reply_kernel,
        [second, precond, spill_low, recv],
        [shape(3 * count, 128), shape(6, NODES)],
        name="reply",
    )
    back = exchange(send, 3, count)
    base, mid, factors = call(
        sweep_kernel,
        [mesh_disp, kappa, low_field, low_kappa, high_field, high_kappa],
        [shape(3, depth, height, across), shape(3, depth, 16, across), shape(depth + 2, 16, across)],
        [
            pltpu.VMEM((depth + 4, height, across), F32),
            pltpu.VMEM((3, depth + 4, height, across), F32),
            pltpu.VMEM((3, depth + 2, height, across), F32),
            pltpu.VMEM((3, depth, height, across), F32),
            pltpu.SemaphoreType.DMA((6,)),
            pltpu.SemaphoreType.DMA,
        ],
        any_ins=range(6),
        any_outs=(0,),
        name="sweep",
    )
    (field,) = call(
        lambda *refs: finish_kernel(slabs, *refs),
        [back, place, low_place, high_place, factors, mid, base],
        [shape(3, depth, height, across)],
        [pltpu.VMEM((3, depth, 16, across), F32), pltpu.SemaphoreType.DMA],
        aliases={6: 0},
        any_ins=(6,),
        any_outs=(0,),
        name="finish",
    )
    return (field, shell_disp)


def solution(mesh):
    in_specs = (
        P(None, ("grp", "slab"), None),
        P(None, ("grp", "slab"), None),
        P(None, ("grp", "slab"), None, None),
        P(("grp", "slab"), None, None),
        P(("grp", "slab"), None),
        P(("grp", "slab")),
        P(None, None, ("grp", "slab")),
        P(None, ("grp", "slab")),
        P(None, ("grp", "slab")),
    )
    out_specs = (P(None, ("grp", "slab"), None, None), P(None, ("grp", "slab")))
    return jax.shard_map(
        on_device, mesh=mesh, in_specs=in_specs, out_specs=out_specs, check_vma=False
    )
```

```python
import jax
import jax.numpy as jnp
from jax import lax
from jax.experimental import pallas as pl
from jax.experimental.pallas import tpu as pltpu
from jax.sharding import PartitionSpec as P

F32 = jnp.float32
BF16 = jnp.bfloat16
AXES = ("grp", "slab")
CAP = 32
NB = 128
NODES = 1024
EXT = NODES + NB
NBLK = EXT // 128
ELEMS = 1024
LOW = 56
VMEM = pl.BlockSpec(memory_space=pltpu.VMEM)
ANY = pl.BlockSpec(memory_space=pl.ANY)
HBM = pl.BlockSpec(memory_space=pltpu.HBM)
MIB = 1024 * 1024


def nn(a, b):
    return lax.dot_general(a, b, (((1,), (0,)), ((), ())), preferred_element_type=F32)


def nt(a, b):
    return lax.dot_general(a, b, (((1,), (1,)), ((), ())), preferred_element_type=F32)


def split(x):
    high = x.astype(BF16).astype(F32)
    return high, x - high


def iota(shape, dim):
    return lax.broadcasted_iota(jnp.int32, shape, dim)


def hot(mask):
    return jnp.where(mask, 1.0, 0.0).astype(F32)


def cat(parts, axis):
    return jnp.concatenate(parts, axis=axis)


def fetch(sems, *pairs):
    copies = [pltpu.make_async_copy(src, dst, sems.at[i]) for i, (src, dst) in enumerate(pairs)]
    for copy in copies:
        copy.start()
    for copy in copies:
        copy.wait()


def pack_kernel(slabs, pp_in, nm_in, own_in, nod_in, send, place, pp, nm, own, nod, sems):
    fetch(sems, (own_in, own), (nod_in, nod), (pp_in, pp), (nm_in, nm))
    owners = own[...]
    nodes = nod[...].astype(F32)
    depth = pp.shape[1]

    def layer(a, z):
        return cat([a[2 * z : 2 * z + 1], a[2 * z + 1 : 2 * z + 2]], 1)

    ow = [layer(owners, z) for z in range(depth)]
    nd = [layer(nodes, z) for z in range(depth)]
    ids = iota((slabs, 256), 0)
    member = [hot(ow[z] == ids) for z in range(depth)]
    before = hot(iota((256, 256), 0) < iota((256, 256), 1)).astype(BF16)
    counts = nn(cat(member, 0).astype(BF16), before)
    offset = jnp.zeros((slabs, 1), F32)
    slot = iota((4 * CAP, 256), 0)
    rank_row = (slot // 4).astype(F32)
    comp = slot % 4
    words = []
    for z in range(depth):
        seen = counts[slabs * z : slabs * (z + 1)] + offset
        rank = jnp.sum(member[z] * seen, axis=0, keepdims=True)
        offset = offset + jnp.sum(member[z], axis=1, keepdims=True)
        place[z : z + 1] = ow[z].astype(F32) * CAP + rank
        jump = pp[0, z : z + 1] - pp[1, z : z + 1]
        t0, t1, t2 = [jump * nm[c, z : z + 1] for c in range(3)]
        value = jnp.where(comp == 0, t0, jnp.where(comp == 1, t1, jnp.where(comp == 2, t2, nd[z])))
        words.append(jnp.where(rank == rank_row, value, 0.0))
    place[depth:8] = jnp.zeros((8 - depth, 256), F32)
    high, low = split(cat(words, 1))
    members = cat(member, 1).astype(BF16)
    packed = nt(members, high.astype(BF16)) + nt(members, low.astype(BF16))
    ahead = cat([packed[1:], jnp.zeros((1, 4 * CAP), F32)], 0)
    first = send.shape[0] - 2 * slabs
    send[0:first] = jnp.zeros((first, 128), F32)
    send[pl.ds(first, slabs, stride=2), :] = packed
    send[pl.ds(first + 1, slabs, stride=2), :] = ahead


def stage_kernel(field, kappa, place, stiffness, conn_in, precond_in, up, down, held, conn, precond, table, sems):
    depth = field.shape[1]
    rows = field.shape[2]
    pairs = [(conn_in, conn), (precond_in, precond), (stiffness, held)]
    for out, start in ((up, depth - 2), (down, 0)):
        for l in range(2):
            for c in range(3):
                row = (2 * c + l) * rows
                pairs.append((field.at[c, start + l], out.at[row : row + rows]))
            row = (6 + l) * rows
            pairs.append((kappa.at[start + l], out.at[row : row + rows]))
    edges = place[...]
    fill = jnp.zeros((7, edges.shape[1]), F32)
    up[8 * rows : 8 * rows + 8] = cat([edges[depth - 1 : depth], fill], 0)
    down[8 * rows : 8 * rows + 8] = cat([edges[0:1], fill], 0)
    fetch(sems, *pairs)
    connect(corners(conn), table)


def corners(conn):
    return [conn[a : a + 1] for a in range(4)]


def connect(nodes, table):
    for a in range(4):
        table[:, a * ELEMS : (a + 1) * ELEMS] = hot(iota((128, ELEMS), 0) == (nodes[a] & 127)).astype(BF16)


def stiff(values, blocks, stiffness, table, spread):
    high, low = split(values)
    parts = []
    for b in range(NBLK):
        lanes = slice(128 * b, 128 * b + 128)
        parts += [high[:, lanes], low[:, lanes]]
    stack = cat(parts, 0).astype(BF16)
    gathered = []
    for a in range(4):
        wide = nn(stack, table[:, a * ELEMS : (a + 1) * ELEMS])
        total = jnp.zeros((8, ELEMS), F32)
        for b in range(NBLK):
            row = wide[16 * b : 16 * b + 8] + wide[16 * b + 8 : 16 * b + 16]
            total = total + jnp.where(blocks[a] == b, row, 0.0)
        gathered.append(total)
    chunk = 256
    pieces = []
    for e in range(0, ELEMS, chunk):
        acc = jnp.zeros((24, chunk), F32)
        for a in range(4):
            for c in range(6):
                acc = acc + stiffness[a * 6 + c, :, e : e + chunk] * gathered[a][c : c + 1, e : e + chunk]
        pieces.append(acc)
    force = cat(pieces, 1)
    for a in range(4):
        part = cat([force[6 * a : 6 * a + 6], jnp.zeros((2, ELEMS), F32)], 0)
        both = cat(split(part), 0)
        for b in range(NBLK):
            spread[16 * b : 16 * b + 16, a * ELEMS : (a + 1) * ELEMS] = jnp.where(
                blocks[a] == b, both, 0.0
            ).astype(BF16)
    summed = nt(spread[...], table[...])
    return cat([summed[16 * b : 16 * b + 8] + summed[16 * b + 8 : 16 * b + 16] for b in range(NBLK)], 1)


def fold(tile):
    both = tile + pltpu.roll(tile, 4, 0)
    return jnp.where(iota(tile.shape, 0) < 3, both, 0.0)


def diagonal(precond, ghost):
    return cat([cat([precond[...], jnp.zeros((2, NODES), F32)], 0), ghost[...]], 1)


def load_kernel(recv, precond, ghost, conn, held, table, load, first, partial, spill, edge, marks, spread, slots):
    blocks = [n >> 7 for n in corners(conn)]
    senders = recv.shape[0] // 2
    ids = iota((128, senders), 0).astype(F32)
    for which in (1, 0):
        data = recv[pl.ds(which, senders, stride=2), :].T
        high, low = split(data)
        for r in range(CAP):
            lanes = slice(r * senders, (r + 1) * senders)
            node = data[4 * r + 3 : 4 * r + 4]
            both = cat([high[4 * r : 4 * r + 4], low[4 * r : 4 * r + 4]], 0)
            if which == 0:
                block = jnp.floor(node * (1.0 / 128.0))
                node = node - 128.0 * block
                for b in range(0, 8, 2):
                    slots[8 * b : 8 * b + 16, lanes] = cat(
                        [jnp.where(block == b + k, both, 0.0) for k in range(2)], 0
                    ).astype(BF16)
            else:
                slots[0:16, lanes] = cat([both, jnp.zeros_like(both)], 0).astype(BF16)
            marks[:, lanes] = hot(ids == node).astype(BF16)
        if which == 0:
            found = nt(slots[...], marks[...])
            sums = [fold(found[8 * b : 8 * b + 8]) for b in range(8)] + sums
        else:
            sums = [fold(nt(slots[0:16], marks[...])[0:8])]
    loading = cat(sums, 1)
    start = diagonal(precond, ghost) * loading
    load[...] = loading
    first[...] = start
    result = stiff(start, blocks, held, table, spread)
    partial[...] = result
    spill[...] = result[:, NODES:]
    edge[...] = result[:, :NB]


def step_kernel(load, first, partial, from_low, from_high, precond, ghost, conn, held, table, second, spill, spread):
    blocks = [n >> 7 for n in corners(conn)]
    scale = diagonal(precond, ghost)
    loading = load[...]
    extra = cat([from_low[...], jnp.zeros((8, NODES - NB), F32), from_high[...]], 1)
    values = first[...] + scale * (loading - (partial[...] + extra))
    result = stiff(values, blocks, held, table, spread)
    own = values + scale * (loading - result)
    second[...] = own[:, :NODES]
    spill[...] = result[:, NODES:]


def reply_kernel(second, precond, from_low, recv, marks, send, shell):
    shift = precond[:, :NB] * from_low[0:6]
    near = second[:, :NB] - cat([shift, jnp.zeros((2, NB), F32)], 0)
    values = cat([near, second[:, NB:]], 1)
    shell[...] = values[0:6]
    high, low = split(values)
    senders = recv.shape[0] // 2
    stack = cat(
        [
            part[0:4, 128 * b : 128 * b + 128]
            for b in range(NODES // 128)
            for part in (high, low)
        ],
        0,
    ).astype(BF16)
    data = recv[pl.ds(0, senders, stride=2), :].T
    upper = iota((8, senders), 0) < 4
    tiles = []
    for t in range(CAP // 2):
        pair = []
        for r in (2 * t, 2 * t + 1):
            node = data[4 * r + 3 : 4 * r + 4]
            block = jnp.floor(node * (1.0 / 128.0))
            wide = nn(stack, marks[:, r * senders : (r + 1) * senders])
            total = jnp.zeros((8, senders), F32)
            for b in range(NODES // 128):
                total = total + jnp.where(block == b, wide[8 * b : 8 * b + 8], 0.0)
            pair.append(total + pltpu.roll(total, 4, 0))
        tiles.append(jnp.where(upper, pair[0], pair[1]))
    answer = cat(tiles, 0).T
    send[pl.ds(0, senders, stride=3), :] = cat([answer[senders - 1 :], answer[: senders - 1]], 0)
    send[pl.ds(1, senders, stride=3), :] = answer
    send[pl.ds(2, senders, stride=3), :] = cat([answer[1:], answer[:1]], 0)


def sweep_kernel(field, kappa, place, low, high, out, mid, factors, places,
                 kext, fext, mext, done, edges, sems, out_sems):
    depth = field.shape[1]
    rows, cols = field.shape[2:]
    level = rows // 2
    flat = lax.axis_index("grp") * lax.axis_size("slab") + lax.axis_index("slab")
    last = lax.axis_size("grp") * lax.axis_size("slab") - 1
    pairs = [(kappa, kext.at[2 : depth + 2]), (field, fext.at[:, 2 : depth + 2])]
    for side, (message, start) in enumerate(((low, 0), (high, depth + 2))):
        pairs.append((message.at[8 * rows : 8 * rows + 8], edges.at[side]))
        for l in range(2):
            for c in range(3):
                row = (2 * c + l) * rows
                pairs.append((message.at[row : row + rows], fext.at[c, start + l]))
            row = (6 + l) * rows
            pairs.append((message.at[row : row + rows], kext.at[start + l]))
    fetch(sems, *pairs)
    places[...] = cat([edges[0, 0:1], place[0:depth], edges[1, 0:1], jnp.zeros((6 - depth, cols), F32)], 0)

    @pl.when(flat == 0)
    def _():
        kext[1] = kext[2]

    @pl.when(flat == last)
    def _():
        kext[depth + 2] = kext[depth + 1]

    row = iota((rows, cols), 0)
    col = iota((rows, cols), 1)

    def weights(l):
        k = kext[l]
        down = k + jnp.where(row == 0, k, pltpu.roll(k, 1, 0))
        up = k + jnp.where(row == rows - 1, k, pltpu.roll(k, rows - 1, 0))
        left = k + jnp.where(col == 0, k, pltpu.roll(k, 1, 1))
        right = k + jnp.where(col == cols - 1, k, pltpu.roll(k, cols - 1, 1))
        back = k + kext[l - 1]
        front = k + kext[l + 1]
        inverse = 1.0 / (down + up + left + right + back + front)
        return (
            jnp.where(row == 0, 0.0, down) * inverse,
            jnp.where(row == rows - 1, 0.0, up) * inverse,
            jnp.where(col == 0, 0.0, left) * inverse,
            jnp.where(col == cols - 1, 0.0, right) * inverse,
            back * inverse,
            front * inverse,
        )

    def blend(w, here, before, after):
        down, up, left, right, back, front = w
        total = down * pltpu.roll(here, 1, 0) + up * pltpu.roll(here, rows - 1, 0)
        total = total + left * pltpu.roll(here, 1, 1) + right * pltpu.roll(here, cols - 1, 1)
        total = total + back * before + front * after
        return jnp.where(row == level, 0.0, total)

    fext[:, :, level : level + 1, :] = jnp.zeros((3, depth + 4, 1, cols), F32)

    def first_sweep(i, carry):
        l = i + 1
        w = weights(l)
        down, up, left, right, back, front = w
        outside = jnp.logical_or(
            jnp.logical_and(flat == 0, i == 0), jnp.logical_and(flat == last, i == depth + 1)
        )
        keep = jnp.where(outside, 0.0, 1.0)
        a, b = level - 1, level - 2
        c, d = level + 1, level + 2
        picked = [
            up[a : a + 1] * keep, back[a : a + 1], front[a : a + 1], left[a : a + 1], right[a : a + 1],
            up[b : b + 1],
            down[c : c + 1] * keep, back[c : c + 1], front[c : c + 1], left[c : c + 1], right[c : c + 1],
            down[d : d + 1],
        ]
        factors[i] = cat(picked + [jnp.zeros((4, cols), F32)], 0)
        for comp in range(3):
            mext[comp, i] = blend(w, fext[comp, l], fext[comp, l - 1], fext[comp, l + 1]) * keep
        return carry

    lax.fori_loop(0, depth + 2, first_sweep, 0)

    def second_sweep(z, carry):
        w = weights(z + 2)
        for comp in range(3):
            value = blend(w, mext[comp, z + 1], mext[comp, z], mext[comp, z + 2])
            done[comp, z] = value
            mid[comp, z] = value[LOW : LOW + 16]

    stores = []
    for z in range(depth):
        second_sweep(z, 0)
        stores.append(pltpu.make_async_copy(done.at[:, z], out.at[:, z], out_sems.at[z]))
        stores[z].start()
    for store in stores:
        store.wait()


def finish_kernel(slabs, recv, places, factors, mid, base, out, rows16, sem):
    depth = mid.shape[1]
    cols = mid.shape[3]
    first = recv.shape[0] - 3 * slabs
    slot = iota((4 * CAP, cols), 0)
    rank_row = (slot // 4).astype(F32)
    ids = iota((slabs, cols), 0).astype(F32)
    views = []
    for j in range(3):
        part = recv[pl.ds(first + j, slabs, stride=3), :]
        views.append(cat(split(part), 0).T.astype(BF16))
    sources = [(j, places[i : i + 1]) for i, j in enumerate([0] + [1] * depth + [2])]
    motion = []
    for j, where in sources:
        owner = jnp.floor(where * (1.0 / CAP))
        rank = where - CAP * owner
        member = hot(owner == ids).astype(BF16)
        wide = nn(views[j], cat([member, member], 0))
        kept = jnp.where(rank == rank_row, wide, 0.0)
        total = kept[0:8]
        for t in range(1, 4 * CAP // 8):
            total = total + kept[8 * t : 8 * t + 8]
        motion.append(total + pltpu.roll(total, 4, 0))
    f = factors
    near = [[f[i, 6 * s : 6 * s + 1] * motion[i] for i in range(depth + 2)] for s in range(2)]
    for z in range(depth):
        i = z + 1
        added = []
        for s in range(2):
            o = 6 * s
            d = near[s]
            side = (
                f[i, o + 1 : o + 2] * d[i - 1]
                + f[i, o + 2 : o + 3] * d[i + 1]
                + f[i, o + 3 : o + 4] * pltpu.roll(d[i], 1, 1)
                + f[i, o + 4 : o + 5] * pltpu.roll(d[i], cols - 1, 1)
                + d[i]
            )
            added.append((side, f[i, o + 5 : o + 6] * d[i]))
        (below, below2), (above, above2) = added
        for comp in range(3):
            k = slice(comp, comp + 1)
            change = cat(
                [jnp.zeros((6, cols), F32), below2[k], below[k], motion[i][k], above[k], above2[k],
                 jnp.zeros((5, cols), F32)], 0
            )
            rows16[comp, z] = mid[comp, z] + change
    store = pltpu.make_async_copy(rows16, out.at[:, :, LOW : LOW + 16, :], sem)
    store.start()
    store.wait()


def shape(*dims):
    return jax.ShapeDtypeStruct(dims, F32)


def call(kernel, ins, outs, scratch, mib=8, aliases=None, name=None):
    kinds = {"v": VMEM, "h": HBM, "a": ANY}
    into, out = name.split("_")[1:]
    return pl.pallas_call(
        kernel,
        out_shape=outs,
        in_specs=[kinds[k] for k in into],
        out_specs=[kinds[k] for k in out],
        scratch_shapes=list(scratch),
        input_output_aliases=aliases or {},
        compiler_params=pltpu.CompilerParams(vmem_limit_bytes=mib * MIB),
        name=name,
    )(*ins)


def exchange(rows, per, count):
    flat = rows.reshape(count, 1, per * 128)
    return lax.all_to_all(flat, AXES, 0, 0, tiled=True).reshape(count * per, 128)


def on_device(
    pressure_pair, normals, mesh_disp, kappa, face_owner, face_node, stiffness, shell_conn, precond
):
    groups = lax.axis_size("grp")
    slabs = lax.axis_size("slab")
    count = groups * slabs
    depth, height, across = mesh_disp.shape[1:]
    up = [(i, i + 1) for i in range(count - 1)]
    down = [(b, a) for a, b in up]
    shell = count - slabs
    shell_up = [(shell + i, shell + i + 1) for i in range(slabs - 1)]
    shell_down = [(b, a) for a, b in shell_up]
    dma = pltpu.SemaphoreType.DMA

    send, place = call(
        lambda *refs: pack_kernel(slabs, *refs),
        [pressure_pair, normals, face_owner.reshape(8, 128), face_node.reshape(8, 128)],
        [shape(2 * count, 128), shape(8, across)],
        [
            pltpu.VMEM(pressure_pair.shape, F32),
            pltpu.VMEM(normals.shape, F32),
            pltpu.VMEM((8, 128), jnp.int32),
            pltpu.VMEM((8, 128), jnp.int32),
            dma((4,)),
        ],
        mib=60,
        name="pack_hhhh_vv",
    )
    ghost = lax.ppermute(jnp.pad(precond[:, :NB], ((0, 2), (0, 0))), AXES, shell_down)
    recv = exchange(send, 2, count)
    message = shape(8 * height + 8, across)
    to_up, to_down, held, conn, diag, table = call(
        stage_kernel,
        [mesh_disp, kappa, place, stiffness, shell_conn, precond],
        [
            message, message, shape(*stiffness.shape),
            jax.ShapeDtypeStruct(shell_conn.shape, jnp.int32), shape(*precond.shape),
            jax.ShapeDtypeStruct((128, 4 * ELEMS), BF16),
        ],
        [dma((19,))],
        name="stage_hhvhhh_vvvvvv",
    )
    low = lax.ppermute(to_up, AXES, up)
    high = lax.ppermute(to_down, AXES, down)

    spread = pltpu.VMEM((16 * NBLK, 4 * ELEMS), BF16)
    load, first, partial, spill, edge, marks = call(
        load_kernel,
        [recv, diag, ghost, conn, held, table],
        [
            shape(8, EXT), shape(8, EXT), shape(8, EXT), shape(8, NB), shape(8, NB),
            jax.ShapeDtypeStruct((128, count * CAP), BF16),
        ],
        [spread, pltpu.VMEM((64, count * CAP), BF16)],
        mib=20,
        name="load_vvvvvv_vvvvvv",
    )
    spill_low = lax.ppermute(spill, AXES, shell_up)
    edge_high = lax.ppermute(edge, AXES, shell_down)
    second, spill = call(
        step_kernel,
        [load, first, partial, spill_low, edge_high, diag, ghost, conn, held, table],
        [shape(8, NODES), shape(8, NB)],
        [spread],
        mib=16,
        name="step_vvvvvvvvvv_vv",
    )
    spill_low = lax.ppermute(spill, AXES, shell_up)
    send, shell_disp = call(
        reply_kernel,
        [second, diag, spill_low, recv, marks],
        [shape(3 * count, 128), shape(6, NODES)],
        [],
        mib=12,
        name="reply_vvvvv_vv",
    )
    back = exchange(send, 3, count)
    base, mid, factors, places = call(
        sweep_kernel,
        [mesh_disp, kappa, place, low, high],
        [shape(3, depth, height, across), shape(3, depth, 16, across), shape(depth + 2, 16, across), shape(8, across)],
        [
            pltpu.VMEM((depth + 4, height, across), F32),
            pltpu.VMEM((3, depth + 4, height, across), F32),
            pltpu.VMEM((3, depth + 2, height, across), F32),
            pltpu.VMEM((3, depth, height, across), F32),
            pltpu.VMEM((2, 8, across), F32),
            dma((20,)),
            dma((depth,)),
        ],
        mib=16,
        name="sweep_hhvaa_hvvv",
    )
    (field,) = call(
        lambda *refs: finish_kernel(slabs, *refs),
        [back, places, factors, mid, base],
        [shape(3, depth, height, across)],
        [pltpu.VMEM((3, depth, 16, across), F32), dma],
        aliases={4: 0},
        name="finish_vvvvh_h",
    )
    return (field, shell_disp)


def solution(mesh):
    in_specs = (
        P(None, ("grp", "slab"), None),
        P(None, ("grp", "slab"), None),
        P(None, ("grp", "slab"), None, None),
        P(("grp", "slab"), None, None),
        P(("grp", "slab"), None),
        P(("grp", "slab")),
        P(None, None, ("grp", "slab")),
        P(None, ("grp", "slab")),
        P(None, ("grp", "slab")),
    )
    out_specs = (P(None, ("grp", "slab"), None, None), P(None, ("grp", "slab")))
    return jax.shard_map(
        on_device, mesh=mesh, in_specs=in_specs, out_specs=out_specs, check_vma=False
    )
```

```python
import jax
import jax.numpy as jnp
from jax import lax
from jax.experimental import pallas as pl
from jax.experimental.pallas import tpu as pltpu
from jax.sharding import PartitionSpec as P

F32 = jnp.float32
BF16 = jnp.bfloat16
AXES = ("grp", "slab")
CAP = 32
NB = 128
NODES = 1024
EXT = NODES + NB
NBLK = EXT // 128
ELEMS = 1024
LOW = 56
VMEM = pl.BlockSpec(memory_space=pltpu.VMEM)
ANY = pl.BlockSpec(memory_space=pl.ANY)
HBM = pl.BlockSpec(memory_space=pltpu.HBM)
MIB = 1024 * 1024


def nn(a, b):
    return lax.dot_general(a, b, (((1,), (0,)), ((), ())), preferred_element_type=F32)


def nt(a, b):
    return lax.dot_general(a, b, (((1,), (1,)), ((), ())), preferred_element_type=F32)


def split(x):
    high = x.astype(BF16).astype(F32)
    return high, x - high


def iota(shape, dim):
    return lax.broadcasted_iota(jnp.int32, shape, dim)


def hot(mask):
    return jnp.where(mask, 1.0, 0.0).astype(F32)


def cat(parts, axis):
    return jnp.concatenate(parts, axis=axis)


def start(sems, *pairs):
    copies = [pltpu.make_async_copy(src, dst, sems.at[i]) for i, (src, dst) in enumerate(pairs)]
    for copy in copies:
        copy.start()
    return copies


def finish(copies):
    for copy in copies:
        copy.wait()


def fetch(sems, *pairs):
    finish(start(sems, *pairs))


def pack_kernel(slabs, pp_in, nm_in, own_in, nod_in, field, kappa, send, place, up, down,
                pp, nm, own, nod, bulk, edges, sems, bulk_sems, out_sems):
    rows = field.shape[2]
    first_layers = (field.shape[1] - 2, 0)
    small = start(sems, (own_in, own), (nod_in, nod), (pp_in, pp), (nm_in, nm))
    loads = []
    for side, z in enumerate(first_layers):
        loads += start(
            bulk_sems.at[side],
            (field.at[:, pl.ds(z, 2)], bulk.at[side, 0:3]),
            (kappa.at[pl.ds(z, 2)], bulk.at[side, 3]),
        )
    finish(small)
    owners = own[...]
    nodes = nod[...].astype(F32)
    depth = pp.shape[1]

    def layer(a, z):
        return cat([a[2 * z : 2 * z + 1], a[2 * z + 1 : 2 * z + 2]], 1)

    ow = [layer(owners, z) for z in range(depth)]
    nd = [layer(nodes, z) for z in range(depth)]
    ids = iota((slabs, 256), 0)
    member = [hot(ow[z] == ids) for z in range(depth)]
    before = hot(iota((256, 256), 0) < iota((256, 256), 1)).astype(BF16)
    counts = nn(cat(member, 0).astype(BF16), before)
    offset = jnp.zeros((slabs, 1), F32)
    slot = iota((4 * CAP, 256), 0)
    rank_row = (slot // 4).astype(F32)
    comp = slot % 4
    words = []
    for z in range(depth):
        seen = counts[slabs * z : slabs * (z + 1)] + offset
        rank = jnp.sum(member[z] * seen, axis=0, keepdims=True)
        offset = offset + jnp.sum(member[z], axis=1, keepdims=True)
        place[z : z + 1] = ow[z].astype(F32) * CAP + rank
        jump = pp[0, z : z + 1] - pp[1, z : z + 1]
        t0, t1, t2 = [jump * nm[c, z : z + 1] for c in range(3)]
        value = jnp.where(comp == 0, t0, jnp.where(comp == 1, t1, jnp.where(comp == 2, t2, nd[z])))
        words.append(jnp.where(rank == rank_row, value, 0.0))
    place[depth:8] = jnp.zeros((8 - depth, 256), F32)
    fill = jnp.zeros((7, 256), F32)
    edges[0] = cat([place[depth - 1 : depth], fill], 0)
    edges[1] = cat([place[0:1], fill], 0)
    finish(loads)
    stores = []
    for side, out in enumerate((up, down)):
        stores += start(
            out_sems.at[side],
            *[(bulk.at[side, c, l], out.at[pl.ds((2 * c + l) * rows, rows)]) for c in range(4) for l in range(2)],
            (edges.at[side], out.at[pl.ds(8 * rows, 8)]),
        )
    high, low = split(cat(words, 1))
    members = cat(member, 1).astype(BF16)
    packed = nt(members, high.astype(BF16)) + nt(members, low.astype(BF16))
    ahead = cat([packed[1:], jnp.zeros((1, 4 * CAP), F32)], 0)
    first = send.shape[0] - 2 * slabs
    send[0:first] = jnp.zeros((first, 128), F32)
    send[pl.ds(first, slabs, stride=2), :] = packed
    send[pl.ds(first + 1, slabs, stride=2), :] = ahead
    finish(stores)


def stage_kernel(stiffness, conn_in, precond_in, held, conn, precond, table, sems):
    copies = start(sems, (conn_in, conn), (precond_in, precond), (stiffness, held))
    finish(copies[:1])
    connect(corners(conn), table)
    finish(copies[1:])


def corners(conn):
    return [conn[a : a + 1] for a in range(4)]


def connect(nodes, table):
    for a in range(4):
        table[:, a * ELEMS : (a + 1) * ELEMS] = hot(iota((128, ELEMS), 0) == (nodes[a] & 127)).astype(BF16)


def stiff(values, blocks, stiffness, table, spread):
    high, low = split(values)
    parts = []
    for b in range(NBLK):
        lanes = slice(128 * b, 128 * b + 128)
        parts += [high[:, lanes], low[:, lanes]]
    stack = cat(parts, 0).astype(BF16)
    gathered = []
    for a in range(4):
        wide = nn(stack, table[:, a * ELEMS : (a + 1) * ELEMS])
        total = jnp.zeros((8, ELEMS), F32)
        for b in range(NBLK):
            row = wide[16 * b : 16 * b + 8] + wide[16 * b + 8 : 16 * b + 16]
            total = total + jnp.where(blocks[a] == b, row, 0.0)
        gathered.append(total)
    chunk = 256
    pieces = []
    for e in range(0, ELEMS, chunk):
        acc = jnp.zeros((24, chunk), F32)
        for a in range(4):
            for c in range(6):
                acc = acc + stiffness[a * 6 + c, :, e : e + chunk] * gathered[a][c : c + 1, e : e + chunk]
        pieces.append(acc)
    force = cat(pieces, 1)
    for a in range(4):
        part = cat([force[6 * a : 6 * a + 6], jnp.zeros((2, ELEMS), F32)], 0)
        both = cat(split(part), 0)
        for b in range(NBLK):
            spread[16 * b : 16 * b + 16, a * ELEMS : (a + 1) * ELEMS] = jnp.where(
                blocks[a] == b, both, 0.0
            ).astype(BF16)
    summed = nt(spread[...], table[...])
    return cat([summed[16 * b : 16 * b + 8] + summed[16 * b + 8 : 16 * b + 16] for b in range(NBLK)], 1)


def fold(tile):
    both = tile + pltpu.roll(tile, 4, 0)
    return jnp.where(iota(tile.shape, 0) < 3, both, 0.0)


def diagonal(precond, ghost):
    joined = cat([precond[...], ghost[:, :NB]], 1)
    return cat([joined, jnp.zeros((2, EXT), F32)], 0)


def load_kernel(recv, precond, ghost, conn, held, table, load, first, partial, spill, edge, spread, slots, marks):
    blocks = [n >> 7 for n in corners(conn)]
    senders = recv.shape[0] // 2
    ids = iota((128, senders), 0).astype(F32)
    for which in (1, 0):
        data = recv[pl.ds(which, senders, stride=2), :].T
        high, low = split(data)
        for r in range(CAP):
            lanes = slice(r * senders, (r + 1) * senders)
            node = data[4 * r + 3 : 4 * r + 4]
            both = cat([high[4 * r : 4 * r + 4], low[4 * r : 4 * r + 4]], 0)
            if which == 0:
                block = jnp.floor(node * (1.0 / 128.0))
                node = node - 128.0 * block
                for b in range(0, 8, 2):
                    slots[8 * b : 8 * b + 16, lanes] = cat(
                        [jnp.where(block == b + k, both, 0.0) for k in range(2)], 0
                    ).astype(BF16)
            else:
                slots[0:16, lanes] = cat([both, jnp.zeros_like(both)], 0).astype(BF16)
            marks[:, lanes] = hot(ids == node).astype(BF16)
        if which == 0:
            found = nt(slots[...], marks[...])
            sums = [fold(found[8 * b : 8 * b + 8]) for b in range(8)] + sums
        else:
            sums = [fold(nt(slots[0:16], marks[...])[0:8])]
    loading = cat(sums, 1)
    values = diagonal(precond, ghost) * loading
    load[...] = loading
    first[...] = values
    result = stiff(values, blocks, held, table, spread)
    partial[...] = result
    spill[...] = result[:, NODES:]
    edge[...] = result[:, :NB]


def step_kernel(load, first, partial, from_low, from_high, precond, ghost, conn, held, table, second, spill, spread):
    blocks = [n >> 7 for n in corners(conn)]
    scale = diagonal(precond, ghost)
    loading = load[...]
    extra = cat([from_low[...], jnp.zeros((8, NODES - NB), F32), from_high[...]], 1)
    values = first[...] + scale * (loading - (partial[...] + extra))
    result = stiff(values, blocks, held, table, spread)
    own = values + scale * (loading - result)
    second[...] = own[:, :NODES]
    spill[...] = result[:, NODES:]


def reply_kernel(second, precond, from_low, recv, send, shell):
    shift = precond[:, :NB] * from_low[0:6]
    near = second[:, :NB] - cat([shift, jnp.zeros((2, NB), F32)], 0)
    values = cat([near, second[:, NB:]], 1)
    shell[...] = values[0:6]
    high, low = split(values)
    senders = recv.shape[0] // 2
    stack = cat(
        [
            part[0:4, 128 * b : 128 * b + 128]
            for b in range(NODES // 128)
            for part in (high, low)
        ],
        0,
    ).astype(BF16)
    data = recv[pl.ds(0, senders, stride=2), :].T
    ids = iota((128, senders), 0).astype(F32)
    upper = iota((8, senders), 0) < 4
    tiles = []
    for t in range(CAP // 2):
        pair = []
        for r in (2 * t, 2 * t + 1):
            node = data[4 * r + 3 : 4 * r + 4]
            block = jnp.floor(node * (1.0 / 128.0))
            wide = nn(stack, hot(ids == node - 128.0 * block).astype(BF16))
            total = jnp.zeros((8, senders), F32)
            for b in range(NODES // 128):
                total = total + jnp.where(block == b, wide[8 * b : 8 * b + 8], 0.0)
            pair.append(total + pltpu.roll(total, 4, 0))
        tiles.append(jnp.where(upper, pair[0], pair[1]))
    answer = cat(tiles, 0).T
    send[pl.ds(0, senders, stride=3), :] = cat([answer[senders - 1 :], answer[: senders - 1]], 0)
    send[pl.ds(1, senders, stride=3), :] = answer
    send[pl.ds(2, senders, stride=3), :] = cat([answer[1:], answer[:1]], 0)


def sweep_kernel(field, kappa, place, low, high, out, mid, factors, places,
                 kext, fext, mext, done, edges, sems, out_sems):
    depth = field.shape[1]
    rows, cols = field.shape[2:]
    level = rows // 2
    flat = lax.axis_index("grp") * lax.axis_size("slab") + lax.axis_index("slab")
    last = lax.axis_size("grp") * lax.axis_size("slab") - 1
    pairs = [(kappa, kext.at[2 : depth + 2]), (field, fext.at[:, 2 : depth + 2])]
    for side, (message, start) in enumerate(((low, 0), (high, depth + 2))):
        pairs.append((message.at[8 * rows : 8 * rows + 8], edges.at[side]))
        for l in range(2):
            for c in range(3):
                row = (2 * c + l) * rows
                pairs.append((message.at[row : row + rows], fext.at[c, start + l]))
            row = (6 + l) * rows
            pairs.append((message.at[row : row + rows], kext.at[start + l]))
    fetch(sems, *pairs)
    places[...] = cat([edges[0, 0:1], place[0:depth], edges[1, 0:1], jnp.zeros((6 - depth, cols), F32)], 0)

    @pl.when(flat == 0)
    def _():
        kext[1] = kext[2]

    @pl.when(flat == last)
    def _():
        kext[depth + 2] = kext[depth + 1]

    row = iota((rows, cols), 0)
    col = iota((rows, cols), 1)

    def weights(l):
        k = kext[l]
        down = k + jnp.where(row == 0, k, pltpu.roll(k, 1, 0))
        up = k + jnp.where(row == rows - 1, k, pltpu.roll(k, rows - 1, 0))
        left = k + jnp.where(col == 0, k, pltpu.roll(k, 1, 1))
        right = k + jnp.where(col == cols - 1, k, pltpu.roll(k, cols - 1, 1))
        back = k + kext[l - 1]
        front = k + kext[l + 1]
        inverse = 1.0 / (down + up + left + right + back + front)
        return (
            jnp.where(row == 0, 0.0, down) * inverse,
            jnp.where(row == rows - 1, 0.0, up) * inverse,
            jnp.where(col == 0, 0.0, left) * inverse,
            jnp.where(col == cols - 1, 0.0, right) * inverse,
            back * inverse,
            front * inverse,
        )

    def blend(w, here, before, after):
        down, up, left, right, back, front = w
        total = down * pltpu.roll(here, 1, 0) + up * pltpu.roll(here, rows - 1, 0)
        total = total + left * pltpu.roll(here, 1, 1) + right * pltpu.roll(here, cols - 1, 1)
        total = total + back * before + front * after
        return jnp.where(row == level, 0.0, total)

    fext[:, :, level : level + 1, :] = jnp.zeros((3, depth + 4, 1, cols), F32)

    def first_sweep(i, carry):
        l = i + 1
        w = weights(l)
        down, up, left, right, back, front = w
        outside = jnp.logical_or(
            jnp.logical_and(flat == 0, i == 0), jnp.logical_and(flat == last, i == depth + 1)
        )
        keep = jnp.where(outside, 0.0, 1.0)
        a, b = level - 1, level - 2
        c, d = level + 1, level + 2
        picked = [
            up[a : a + 1] * keep, back[a : a + 1], front[a : a + 1], left[a : a + 1], right[a : a + 1],
            up[b : b + 1],
            down[c : c + 1] * keep, back[c : c + 1], front[c : c + 1], left[c : c + 1], right[c : c + 1],
            down[d : d + 1],
        ]
        factors[i] = cat(picked + [jnp.zeros((4, cols), F32)], 0)
        for comp in range(3):
            mext[comp, i] = blend(w, fext[comp, l], fext[comp, l - 1], fext[comp, l + 1]) * keep
        return carry

    lax.fori_loop(0, depth + 2, first_sweep, 0)

    def second_sweep(z, carry):
        w = weights(z + 2)
        for comp in range(3):
            value = blend(w, mext[comp, z + 1], mext[comp, z], mext[comp, z + 2])
            done[comp, z] = value
            mid[comp, z] = value[LOW : LOW + 16]

    stores = []
    for z in range(depth):
        second_sweep(z, 0)
        stores.append(pltpu.make_async_copy(done.at[:, z], out.at[:, z], out_sems.at[z]))
        stores[z].start()
    for store in stores:
        store.wait()


def finish_kernel(slabs, recv, places, factors, mid, base, out, rows16, sem):
    depth = mid.shape[1]
    cols = mid.shape[3]
    first = recv.shape[0] - 3 * slabs
    slot = iota((4 * CAP, cols), 0)
    rank_row = (slot // 4).astype(F32)
    ids = iota((slabs, cols), 0).astype(F32)
    views = []
    for j in range(3):
        part = recv[pl.ds(first + j, slabs, stride=3), :]
        views.append(cat(split(part), 0).T.astype(BF16))
    sources = [(j, places[i : i + 1]) for i, j in enumerate([0] + [1] * depth + [2])]
    motion = []
    for j, where in sources:
        owner = jnp.floor(where * (1.0 / CAP))
        rank = where - CAP * owner
        member = hot(owner == ids).astype(BF16)
        wide = nn(views[j], cat([member, member], 0))
        kept = jnp.where(rank == rank_row, wide, 0.0)
        total = kept[0:8]
        for t in range(1, 4 * CAP // 8):
            total = total + kept[8 * t : 8 * t + 8]
        motion.append(total + pltpu.roll(total, 4, 0))
    f = factors
    near = [[f[i, 6 * s : 6 * s + 1] * motion[i] for i in range(depth + 2)] for s in range(2)]
    for z in range(depth):
        i = z + 1
        added = []
        for s in range(2):
            o = 6 * s
            d = near[s]
            side = (
                f[i, o + 1 : o + 2] * d[i - 1]
                + f[i, o + 2 : o + 3] * d[i + 1]
                + f[i, o + 3 : o + 4] * pltpu.roll(d[i], 1, 1)
                + f[i, o + 4 : o + 5] * pltpu.roll(d[i], cols - 1, 1)
                + d[i]
            )
            added.append((side, f[i, o + 5 : o + 6] * d[i]))
        (below, below2), (above, above2) = added
        for comp in range(3):
            k = slice(comp, comp + 1)
            change = cat(
                [jnp.zeros((6, cols), F32), below2[k], below[k], motion[i][k], above[k], above2[k],
                 jnp.zeros((5, cols), F32)], 0
            )
            rows16[comp, z] = mid[comp, z] + change
    store = pltpu.make_async_copy(rows16, out.at[:, :, LOW : LOW + 16, :], sem)
    store.start()
    store.wait()


def shape(*dims):
    return jax.ShapeDtypeStruct(dims, F32)


def call(kernel, ins, outs, scratch, mib=8, aliases=None, name=None):
    kinds = {"v": VMEM, "h": HBM, "a": ANY}
    into, out = name.split("_")[1:]
    return pl.pallas_call(
        kernel,
        out_shape=outs,
        in_specs=[kinds[k] for k in into],
        out_specs=[kinds[k] for k in out],
        scratch_shapes=list(scratch),
        input_output_aliases=aliases or {},
        compiler_params=pltpu.CompilerParams(vmem_limit_bytes=mib * MIB),
        name=name,
    )(*ins)


def exchange(rows, per, count):
    flat = rows.reshape(count, 1, per * 128)
    return lax.all_to_all(flat, AXES, 0, 0, tiled=True).reshape(count * per, 128)


def on_device(
    pressure_pair, normals, mesh_disp, kappa, face_owner, face_node, stiffness, shell_conn, precond
):
    groups = lax.axis_size("grp")
    slabs = lax.axis_size("slab")
    count = groups * slabs
    depth, height, across = mesh_disp.shape[1:]
    up = [(i, i + 1) for i in range(count - 1)]
    down = [(b, a) for a, b in up]
    shell = count - slabs
    shell_up = [(shell + i, shell + i + 1) for i in range(slabs - 1)]
    shell_down = [(b, a) for a, b in shell_up]
    dma = pltpu.SemaphoreType.DMA

    ghost = lax.ppermute(precond, AXES, shell_down)
    message = shape(8 * height + 8, across)
    send, place, to_up, to_down = call(
        lambda *refs: pack_kernel(slabs, *refs),
        [pressure_pair, normals, face_owner.reshape(8, 128), face_node.reshape(8, 128), mesh_disp, kappa],
        [shape(2 * count, 128), shape(8, across), message, message],
        [
            pltpu.VMEM(pressure_pair.shape, F32),
            pltpu.VMEM(normals.shape, F32),
            pltpu.VMEM((8, 128), jnp.int32),
            pltpu.VMEM((8, 128), jnp.int32),
            pltpu.VMEM((2, 4, 2, height, across), F32),
            pltpu.VMEM((2, 8, across), F32),
            dma((4,)),
            dma((2, 2)),
            dma((2, 9)),
        ],
        mib=63,
        name="pack_hhhhhh_vvhh",
    )
    recv = exchange(send, 2, count)
    low = lax.ppermute(to_up, AXES, up)
    high = lax.ppermute(to_down, AXES, down)

    held, conn, diag, table = call(
        stage_kernel,
        [stiffness, shell_conn, precond],
        [
            shape(*stiffness.shape), jax.ShapeDtypeStruct(shell_conn.shape, jnp.int32), shape(*precond.shape),
            jax.ShapeDtypeStruct((128, 4 * ELEMS), BF16),
        ],
        [dma((3,))],
        name="stage_hhh_vvvv",
    )
    spread = pltpu.VMEM((16 * NBLK, 4 * ELEMS), BF16)
    load, first, partial, spill, edge = call(
        load_kernel,
        [recv, diag, ghost, conn, held, table],
        [shape(8, EXT), shape(8, EXT), shape(8, EXT), shape(8, NB), shape(8, NB)],
        [spread, pltpu.VMEM((64, count * CAP), BF16), pltpu.VMEM((128, count * CAP), BF16)],
        mib=20,
        name="load_vvvvvv_vvvvv",
    )
    spill_low = lax.ppermute(spill, AXES, shell_up)
    edge_high = lax.ppermute(edge, AXES, shell_down)
    second, spill = call(
        step_kernel,
        [load, first, partial, spill_low, edge_high, diag, ghost, conn, held, table],
        [shape(8, NODES), shape(8, NB)],
        [spread],
        mib=16,
        name="step_vvvvvvvvvv_vv",
    )
    spill_low = lax.ppermute(spill, AXES, shell_up)
    send, shell_disp = call(
        reply_kernel,
        [second, diag, spill_low, recv],
        [shape(3 * count, 128), shape(6, NODES)],
        [],
        mib=12,
        name="reply_vvvv_vv",
    )
    back = exchange(send, 3, count)
    base, mid, factors, places = call(
        sweep_kernel,
        [mesh_disp, kappa, place, low, high],
        [shape(3, depth, height, across), shape(3, depth, 16, across), shape(depth + 2, 16, across), shape(8, across)],
        [
            pltpu.VMEM((depth + 4, height, across), F32),
            pltpu.VMEM((3, depth + 4, height, across), F32),
            pltpu.VMEM((3, depth + 2, height, across), F32),
            pltpu.VMEM((3, depth, height, across), F32),
            pltpu.VMEM((2, 8, across), F32),
            dma((20,)),
            dma((depth,)),
        ],
        mib=16,
        name="sweep_hhvaa_hvvv",
    )
    (field,) = call(
        lambda *refs: finish_kernel(slabs, *refs),
        [back, places, factors, mid, base],
        [shape(3, depth, height, across)],
        [pltpu.VMEM((3, depth, 16, across), F32), dma],
        aliases={4: 0},
        name="finish_vvvvh_h",
    )
    return (field, shell_disp)


def solution(mesh):
    in_specs = (
        P(None, ("grp", "slab"), None),
        P(None, ("grp", "slab"), None),
        P(None, ("grp", "slab"), None, None),
        P(("grp", "slab"), None, None),
        P(("grp", "slab"), None),
        P(("grp", "slab")),
        P(None, None, ("grp", "slab")),
        P(None, ("grp", "slab")),
        P(None, ("grp", "slab")),
    )
    out_specs = (P(None, ("grp", "slab"), None, None), P(None, ("grp", "slab")))
    return jax.shard_map(
        on_device, mesh=mesh, in_specs=in_specs, out_specs=out_specs, check_vma=False
    )
```

```python
import jax
import jax.numpy as jnp
from jax import lax
from jax.experimental import pallas as pl
from jax.experimental.pallas import tpu as pltpu
from jax.sharding import PartitionSpec as P

F32 = jnp.float32
BF16 = jnp.bfloat16
AXES = ("grp", "slab")
CAP = 32
NB = 128
NODES = 1024
EXT = NODES + NB
NBLK = EXT // 128
ELEMS = 1024
LOW = 56
VMEM = pl.BlockSpec(memory_space=pltpu.VMEM)
ANY = pl.BlockSpec(memory_space=pl.ANY)
HBM = pl.BlockSpec(memory_space=pltpu.HBM)
MIB = 1024 * 1024


def nn(a, b):
    return lax.dot_general(a, b, (((1,), (0,)), ((), ())), preferred_element_type=F32)


def nt(a, b):
    return lax.dot_general(a, b, (((1,), (1,)), ((), ())), preferred_element_type=F32)


def split(x):
    high = x.astype(BF16).astype(F32)
    return high, x - high


def iota(shape, dim):
    return lax.broadcasted_iota(jnp.int32, shape, dim)


def hot(mask):
    return jnp.where(mask, 1.0, 0.0).astype(F32)


def cat(parts, axis):
    return jnp.concatenate(parts, axis=axis)


def start(sems, *pairs):
    copies = [pltpu.make_async_copy(src, dst, sems.at[i]) for i, (src, dst) in enumerate(pairs)]
    for copy in copies:
        copy.start()
    return copies


def finish(copies):
    for copy in copies:
        copy.wait()


def fetch(sems, *pairs):
    finish(start(sems, *pairs))


def pack_kernel(slabs, pp_in, nm_in, own_in, nod_in, field, kappa, send, place, up, down,
                pp, nm, own, nod, bulk, edges, sems, bulk_sems, out_sems):
    rows = field.shape[2]
    first_layers = (field.shape[1] - 2, 0)
    small = start(sems, (own_in, own), (nod_in, nod), (pp_in, pp), (nm_in, nm))
    loads = []
    for side, z in enumerate(first_layers):
        loads += start(
            bulk_sems.at[side],
            (field.at[:, pl.ds(z, 2)], bulk.at[side, 0:3]),
            (kappa.at[pl.ds(z, 2)], bulk.at[side, 3]),
        )
    finish(small)
    owners = own[...]
    nodes = nod[...].astype(F32)
    depth = pp.shape[1]

    def layer(a, z):
        return cat([a[2 * z : 2 * z + 1], a[2 * z + 1 : 2 * z + 2]], 1)

    ow = [layer(owners, z) for z in range(depth)]
    nd = [layer(nodes, z) for z in range(depth)]
    ids = iota((slabs, 256), 0)
    member = [hot(ow[z] == ids) for z in range(depth)]
    before = hot(iota((256, 256), 0) < iota((256, 256), 1)).astype(BF16)
    counts = nn(cat(member, 0).astype(BF16), before)
    offset = jnp.zeros((slabs, 1), F32)
    slot = iota((4 * CAP, 256), 0)
    rank_row = (slot // 4).astype(F32)
    comp = slot % 4
    words = []
    for z in range(depth):
        seen = counts[slabs * z : slabs * (z + 1)] + offset
        rank = jnp.sum(member[z] * seen, axis=0, keepdims=True)
        offset = offset + jnp.sum(member[z], axis=1, keepdims=True)
        place[z : z + 1] = ow[z].astype(F32) * CAP + rank
        jump = pp[0, z : z + 1] - pp[1, z : z + 1]
        t0, t1, t2 = [jump * nm[c, z : z + 1] for c in range(3)]
        value = jnp.where(comp == 0, t0, jnp.where(comp == 1, t1, jnp.where(comp == 2, t2, nd[z])))
        words.append(jnp.where(rank == rank_row, value, 0.0))
    place[depth:8] = jnp.zeros((8 - depth, 256), F32)
    fill = jnp.zeros((7, 256), F32)
    edges[0] = cat([place[depth - 1 : depth], fill], 0)
    edges[1] = cat([place[0:1], fill], 0)
    finish(loads)
    stores = []
    for side, out in enumerate((up, down)):
        stores += start(
            out_sems.at[side],
            *[(bulk.at[side, c, l], out.at[pl.ds((2 * c + l) * rows, rows)]) for c in range(4) for l in range(2)],
            (edges.at[side], out.at[pl.ds(8 * rows, 8)]),
        )
    high, low = split(cat(words, 1))
    members = cat(member, 1).astype(BF16)
    packed = nt(members, high.astype(BF16)) + nt(members, low.astype(BF16))
    ahead = cat([packed[1:], jnp.zeros((1, 4 * CAP), F32)], 0)
    first = send.shape[0] - 2 * slabs
    send[0:first] = jnp.zeros((first, 128), F32)
    send[pl.ds(first, slabs, stride=2), :] = packed
    send[pl.ds(first + 1, slabs, stride=2), :] = ahead
    finish(stores)


def stage_kernel(stiffness, conn_in, precond_in, held, conn, precond, table, sems):
    copies = start(sems, (conn_in, conn), (precond_in, precond), (stiffness, held))
    finish(copies[:1])
    connect(corners(conn), table)
    finish(copies[1:])


def corners(conn):
    return [conn[a : a + 1] for a in range(4)]


def connect(nodes, table):
    for a in range(4):
        table[:, a * ELEMS : (a + 1) * ELEMS] = hot(iota((128, ELEMS), 0) == (nodes[a] & 127)).astype(BF16)


def stiff(values, blocks, stiffness, table, spread):
    high, low = split(values)
    parts = []
    for b in range(NBLK):
        lanes = slice(128 * b, 128 * b + 128)
        parts += [high[:, lanes], low[:, lanes]]
    stack = cat(parts, 0).astype(BF16)
    gathered = []
    for a in range(4):
        wide = nn(stack, table[:, a * ELEMS : (a + 1) * ELEMS])
        total = jnp.zeros((8, ELEMS), F32)
        for b in range(NBLK):
            row = wide[16 * b : 16 * b + 8] + wide[16 * b + 8 : 16 * b + 16]
            total = total + jnp.where(blocks[a] == b, row, 0.0)
        gathered.append(total)
    chunk = 256
    pieces = []
    for e in range(0, ELEMS, chunk):
        acc = jnp.zeros((24, chunk), F32)
        for a in range(4):
            for c in range(6):
                acc = acc + stiffness[a * 6 + c, :, e : e + chunk] * gathered[a][c : c + 1, e : e + chunk]
        pieces.append(acc)
    force = cat(pieces, 1)
    for a in range(4):
        part = cat([force[6 * a : 6 * a + 6], jnp.zeros((2, ELEMS), F32)], 0)
        both = cat(split(part), 0)
        for b in range(NBLK):
            spread[16 * b : 16 * b + 16, a * ELEMS : (a + 1) * ELEMS] = jnp.where(
                blocks[a] == b, both, 0.0
            ).astype(BF16)
    summed = nt(spread[...], table[...])
    return cat([summed[16 * b : 16 * b + 8] + summed[16 * b + 8 : 16 * b + 16] for b in range(NBLK)], 1)


def fold(tile):
    both = tile + pltpu.roll(tile, 4, 0)
    return jnp.where(iota(tile.shape, 0) < 3, both, 0.0)


def diagonal(precond, ghost):
    joined = cat([precond[...], ghost[:, :NB]], 1)
    return cat([joined, jnp.zeros((2, EXT), F32)], 0)


def load_kernel(recv, precond, ghost, conn, held, table, load, first, partial, spill, edge, kept, spread, slots, marks):
    blocks = [n >> 7 for n in corners(conn)]
    senders = recv.shape[0] // 2
    ids = iota((128, senders), 0).astype(F32)
    for which in (1, 0):
        data = recv[pl.ds(which, senders, stride=2), :].T
        if which == 0:
            kept[...] = data
        high, low = split(data)
        for r in range(CAP):
            lanes = slice(r * senders, (r + 1) * senders)
            node = data[4 * r + 3 : 4 * r + 4]
            both = cat([high[4 * r : 4 * r + 4], low[4 * r : 4 * r + 4]], 0)
            if which == 0:
                block = jnp.floor(node * (1.0 / 128.0))
                node = node - 128.0 * block
                for b in range(0, 8, 2):
                    slots[8 * b : 8 * b + 16, lanes] = cat(
                        [jnp.where(block == b + k, both, 0.0) for k in range(2)], 0
                    ).astype(BF16)
            else:
                slots[0:16, lanes] = cat([both, jnp.zeros_like(both)], 0).astype(BF16)
            marks[:, lanes] = hot(ids == node).astype(BF16)
        if which == 0:
            found = nt(slots[...], marks[...])
            sums = [fold(found[8 * b : 8 * b + 8]) for b in range(8)] + sums
        else:
            sums = [fold(nt(slots[0:16], marks[...])[0:8])]
    loading = cat(sums, 1)
    values = diagonal(precond, ghost) * loading
    load[...] = loading
    first[...] = values
    result = stiff(values, blocks, held, table, spread)
    partial[...] = result
    spill[...] = result[:, NODES:]
    edge[...] = result[:, :NB]


def step_kernel(load, first, partial, from_low, from_high, precond, ghost, conn, held, table, second, spill, spread):
    blocks = [n >> 7 for n in corners(conn)]
    scale = diagonal(precond, ghost)
    loading = load[...]
    extra = cat([from_low[...], jnp.zeros((8, NODES - NB), F32), from_high[...]], 1)
    values = first[...] + scale * (loading - (partial[...] + extra))
    result = stiff(values, blocks, held, table, spread)
    own = values + scale * (loading - result)
    second[...] = own[:, :NODES]
    spill[...] = result[:, NODES:]


def reply_kernel(second, precond, from_low, data, swept, send, shell):
    shift = precond[:, :NB] * from_low[0:6]
    near = second[:, :NB] - cat([shift, jnp.zeros((2, NB), F32)], 0)
    values = cat([near, second[:, NB:]], 1)
    shell[...] = values[0:6]
    high, low = split(values)
    senders = data.shape[1]
    stack = cat(
        [
            part[0:4, 128 * b : 128 * b + 128]
            for b in range(NODES // 128)
            for part in (high, low)
        ],
        0,
    ).astype(BF16)
    data = data[...]
    ids = iota((128, senders), 0).astype(F32)
    upper = iota((8, senders), 0) < 4
    tiles = []
    for t in range(CAP // 2):
        pair = []
        for r in (2 * t, 2 * t + 1):
            node = data[4 * r + 3 : 4 * r + 4]
            block = jnp.floor(node * (1.0 / 128.0))
            wide = nn(stack, hot(ids == node - 128.0 * block).astype(BF16))
            total = jnp.zeros((8, senders), F32)
            for b in range(NODES // 128):
                total = total + jnp.where(block == b, wide[8 * b : 8 * b + 8], 0.0)
            pair.append(total + pltpu.roll(total, 4, 0))
        tiles.append(jnp.where(upper, pair[0], pair[1]))
    answer = cat(tiles, 0).T
    send[pl.ds(0, senders, stride=3), :] = cat([answer[senders - 1 :], answer[: senders - 1]], 0)
    send[pl.ds(1, senders, stride=3), :] = answer
    send[pl.ds(2, senders, stride=3), :] = cat([answer[1:], answer[:1]], 0)


def sweep_kernel(field, kappa, place, low, high, out, mid, factors, places,
                 kext, fext, mext, done, edges, sems, out_sems):
    depth = field.shape[1]
    rows, cols = field.shape[2:]
    level = rows // 2
    flat = lax.axis_index("grp") * lax.axis_size("slab") + lax.axis_index("slab")
    last = lax.axis_size("grp") * lax.axis_size("slab") - 1
    pairs = [(kappa, kext.at[2 : depth + 2]), (field, fext.at[:, 2 : depth + 2])]
    for side, (message, start) in enumerate(((low, 0), (high, depth + 2))):
        pairs.append((message.at[8 * rows : 8 * rows + 8], edges.at[side]))
        for l in range(2):
            for c in range(3):
                row = (2 * c + l) * rows
                pairs.append((message.at[row : row + rows], fext.at[c, start + l]))
            row = (6 + l) * rows
            pairs.append((message.at[row : row + rows], kext.at[start + l]))
    fetch(sems, *pairs)
    places[...] = cat([edges[0, 0:1], place[0:depth], edges[1, 0:1], jnp.zeros((6 - depth, cols), F32)], 0)

    @pl.when(flat == 0)
    def _():
        kext[1] = kext[2]

    @pl.when(flat == last)
    def _():
        kext[depth + 2] = kext[depth + 1]

    row = iota((rows, cols), 0)
    col = iota((rows, cols), 1)

    def weights(l):
        k = kext[l]
        down = k + jnp.where(row == 0, k, pltpu.roll(k, 1, 0))
        up = k + jnp.where(row == rows - 1, k, pltpu.roll(k, rows - 1, 0))
        left = k + jnp.where(col == 0, k, pltpu.roll(k, 1, 1))
        right = k + jnp.where(col == cols - 1, k, pltpu.roll(k, cols - 1, 1))
        back = k + kext[l - 1]
        front = k + kext[l + 1]
        inverse = 1.0 / (down + up + left + right + back + front)
        return (
            jnp.where(row == 0, 0.0, down) * inverse,
            jnp.where(row == rows - 1, 0.0, up) * inverse,
            jnp.where(col == 0, 0.0, left) * inverse,
            jnp.where(col == cols - 1, 0.0, right) * inverse,
            back * inverse,
            front * inverse,
        )

    def blend(w, here, before, after):
        down, up, left, right, back, front = w
        total = down * pltpu.roll(here, 1, 0) + up * pltpu.roll(here, rows - 1, 0)
        total = total + left * pltpu.roll(here, 1, 1) + right * pltpu.roll(here, cols - 1, 1)
        total = total + back * before + front * after
        return jnp.where(row == level, 0.0, total)

    fext[:, :, level : level + 1, :] = jnp.zeros((3, depth + 4, 1, cols), F32)

    def first_sweep(i, carry):
        l = i + 1
        w = weights(l)
        down, up, left, right, back, front = w
        outside = jnp.logical_or(
            jnp.logical_and(flat == 0, i == 0), jnp.logical_and(flat == last, i == depth + 1)
        )
        keep = jnp.where(outside, 0.0, 1.0)
        a, b = level - 1, level - 2
        c, d = level + 1, level + 2
        picked = [
            up[a : a + 1] * keep, back[a : a + 1], front[a : a + 1], left[a : a + 1], right[a : a + 1],
            up[b : b + 1],
            down[c : c + 1] * keep, back[c : c + 1], front[c : c + 1], left[c : c + 1], right[c : c + 1],
            down[d : d + 1],
        ]
        factors[i] = cat(picked + [jnp.zeros((4, cols), F32)], 0)
        for comp in range(3):
            mext[comp, i] = blend(w, fext[comp, l], fext[comp, l - 1], fext[comp, l + 1]) * keep
        return carry

    lax.fori_loop(0, depth + 2, first_sweep, 0)

    def second_sweep(z):
        w = weights(z + 2)
        for comp in range(3):
            value = blend(w, mext[comp, z + 1], mext[comp, z], mext[comp, z + 2])
            done[comp, z] = value
            mid[comp, z] = value[LOW : LOW + 16]

    stores = []
    for z in range(depth):
        second_sweep(z)
        stores.append(pltpu.make_async_copy(done.at[:, z], out.at[:, z], out_sems.at[z]))
        stores[z].start()
    for store in stores:
        store.wait()


def finish_kernel(slabs, recv, places, factors, mid, base, out, rows16, sem):
    depth = mid.shape[1]
    cols = mid.shape[3]
    first = recv.shape[0] - 3 * slabs
    slot = iota((4 * CAP, cols), 0)
    rank_row = (slot // 4).astype(F32)
    ids = iota((slabs, cols), 0).astype(F32)
    views = []
    for j in range(3):
        part = recv[pl.ds(first + j, slabs, stride=3), :]
        views.append(cat(split(part), 0).T.astype(BF16))
    sources = [(j, places[i : i + 1]) for i, j in enumerate([0] + [1] * depth + [2])]
    motion = []
    for j, where in sources:
        owner = jnp.floor(where * (1.0 / CAP))
        rank = where - CAP * owner
        member = hot(owner == ids).astype(BF16)
        wide = nn(views[j], cat([member, member], 0))
        kept = jnp.where(rank == rank_row, wide, 0.0)
        total = kept[0:8]
        for t in range(1, 4 * CAP // 8):
            total = total + kept[8 * t : 8 * t + 8]
        motion.append(total + pltpu.roll(total, 4, 0))
    f = factors
    near = [[f[i, 6 * s : 6 * s + 1] * motion[i] for i in range(depth + 2)] for s in range(2)]
    for z in range(depth):
        i = z + 1
        added = []
        for s in range(2):
            o = 6 * s
            d = near[s]
            side = (
                f[i, o + 1 : o + 2] * d[i - 1]
                + f[i, o + 2 : o + 3] * d[i + 1]
                + f[i, o + 3 : o + 4] * pltpu.roll(d[i], 1, 1)
                + f[i, o + 4 : o + 5] * pltpu.roll(d[i], cols - 1, 1)
                + d[i]
            )
            added.append((side, f[i, o + 5 : o + 6] * d[i]))
        (below, below2), (above, above2) = added
        for comp in range(3):
            k = slice(comp, comp + 1)
            change = cat(
                [jnp.zeros((6, cols), F32), below2[k], below[k], motion[i][k], above[k], above2[k],
                 jnp.zeros((5, cols), F32)], 0
            )
            rows16[comp, z] = mid[comp, z] + change
    store = pltpu.make_async_copy(rows16, out.at[:, :, LOW : LOW + 16, :], sem)
    store.start()
    store.wait()


def shape(*dims):
    return jax.ShapeDtypeStruct(dims, F32)


def call(kernel, ins, outs, scratch, mib=8, aliases=None, name=None):
    kinds = {"v": VMEM, "h": HBM, "a": ANY}
    into, out = name.split("_")[1:]
    return pl.pallas_call(
        kernel,
        out_shape=outs,
        in_specs=[kinds[k] for k in into],
        out_specs=[kinds[k] for k in out],
        scratch_shapes=list(scratch),
        input_output_aliases=aliases or {},
        compiler_params=pltpu.CompilerParams(vmem_limit_bytes=mib * MIB),
    )(*ins)


def exchange(rows, per, count):
    flat = rows.reshape(count, 1, per * 128)
    return lax.all_to_all(flat, AXES, 0, 0, tiled=True).reshape(count * per, 128)


def on_device(
    pressure_pair, normals, mesh_disp, kappa, face_owner, face_node, stiffness, shell_conn, precond
):
    groups = lax.axis_size("grp")
    slabs = lax.axis_size("slab")
    count = groups * slabs
    depth, height, across = mesh_disp.shape[1:]
    up = [(i, i + 1) for i in range(count - 1)]
    down = [(b, a) for a, b in up]
    shell = count - slabs
    shell_up = [(shell + i, shell + i + 1) for i in range(slabs - 1)]
    shell_down = [(b, a) for a, b in shell_up]
    dma = pltpu.SemaphoreType.DMA

    ghost = lax.ppermute(precond, AXES, shell_down)
    message = shape(8 * height + 8, across)
    send, place, to_up, to_down = call(
        lambda *refs: pack_kernel(slabs, *refs),
        [pressure_pair, normals, face_owner.reshape(8, 128), face_node.reshape(8, 128), mesh_disp, kappa],
        [shape(2 * count, 128), shape(8, across), message, message],
        [
            pltpu.VMEM(pressure_pair.shape, F32),
            pltpu.VMEM(normals.shape, F32),
            pltpu.VMEM((8, 128), jnp.int32),
            pltpu.VMEM((8, 128), jnp.int32),
            pltpu.VMEM((2, 4, 2, height, across), F32),
            pltpu.VMEM((2, 8, across), F32),
            dma((4,)),
            dma((2, 2)),
            dma((2, 9)),
        ],
        mib=63,
        name="pack_hhhhhh_vvhh",
    )
    recv = exchange(send, 2, count)
    low = lax.ppermute(to_up, AXES, up)
    high = lax.ppermute(to_down, AXES, down)

    held, conn, diag, table = call(
        stage_kernel,
        [stiffness, shell_conn, precond],
        [
            shape(*stiffness.shape), jax.ShapeDtypeStruct(shell_conn.shape, jnp.int32), shape(*precond.shape),
            jax.ShapeDtypeStruct((128, 4 * ELEMS), BF16),
        ],
        [dma((3,))],
        name="stage_hhh_vvvv",
    )
    spread = pltpu.VMEM((16 * NBLK, 4 * ELEMS), BF16)
    load, first, partial, spill, edge, kept = call(
        load_kernel,
        [recv, diag, ghost, conn, held, table],
        [shape(8, EXT), shape(8, EXT), shape(8, EXT), shape(8, NB), shape(8, NB), shape(128, count)],
        [spread, pltpu.VMEM((64, count * CAP), BF16), pltpu.VMEM((128, count * CAP), BF16)],
        mib=20,
        name="load_vvvvvv_vvvvvv",
    )
    spill_low = lax.ppermute(spill, AXES, shell_up)
    edge_high = lax.ppermute(edge, AXES, shell_down)
    second, spill = call(
        step_kernel,
        [load, first, partial, spill_low, edge_high, diag, ghost, conn, held, table],
        [shape(8, NODES), shape(8, NB)],
        [spread],
        mib=16,
        name="step_vvvvvvvvvv_vv",
    )
    spill_low = lax.ppermute(spill, AXES, shell_up)
    base, mid, factors, places = call(
        sweep_kernel,
        [mesh_disp, kappa, place, low, high],
        [shape(3, depth, height, across), shape(3, depth, 16, across), shape(depth + 2, 16, across), shape(8, across)],
        [
            pltpu.VMEM((depth + 4, height, across), F32),
            pltpu.VMEM((3, depth + 4, height, across), F32),
            pltpu.VMEM((3, depth + 2, height, across), F32),
            pltpu.VMEM((3, depth, height, across), F32),
            pltpu.VMEM((2, 8, across), F32),
            dma((20,)),
            dma((depth,)),
        ],
        mib=16,
        name="sweep_hhvaa_hvvv",
    )
    send, shell_disp = call(
        reply_kernel,
        [second, diag, spill_low, kept, places],
        [shape(3 * count, 128), shape(6, NODES)],
        [],
        mib=12,
        name="reply_vvvvv_vv",
    )
    back = exchange(send, 3, count)
    (field,) = call(
        lambda *refs: finish_kernel(slabs, *refs),
        [back, places, factors, mid, base],
        [shape(3, depth, height, across)],
        [pltpu.VMEM((3, depth, 16, across), F32), dma],
        aliases={4: 0},
        name="finish_vvvvh_h",
    )
    return (field, shell_disp)


def solution(mesh):
    in_specs = (
        P(None, ("grp", "slab"), None),
        P(None, ("grp", "slab"), None),
        P(None, ("grp", "slab"), None, None),
        P(("grp", "slab"), None, None),
        P(("grp", "slab"), None),
        P(("grp", "slab")),
        P(None, None, ("grp", "slab")),
        P(None, ("grp", "slab")),
        P(None, ("grp", "slab")),
    )
    out_specs = (P(None, ("grp", "slab"), None, None), P(None, ("grp", "slab")))
    return jax.shard_map(
        on_device, mesh=mesh, in_specs=in_specs, out_specs=out_specs, check_vma=False
    )
```

```python
import jax
import jax.numpy as jnp
from jax import lax
from jax.experimental import pallas as pl
from jax.experimental.pallas import tpu as pltpu
from jax.sharding import PartitionSpec as P

F32 = jnp.float32
BF16 = jnp.bfloat16
AXES = ("grp", "slab")
CAP = 32
NB = 128
NODES = 1024
EXT = NODES + NB
NBLK = EXT // 128
ELEMS = 1024
LOW = 56
VMEM = pl.BlockSpec(memory_space=pltpu.VMEM)
ANY = pl.BlockSpec(memory_space=pl.ANY)
HBM = pl.BlockSpec(memory_space=pltpu.HBM)
MIB = 1024 * 1024


def nn(a, b):
    return lax.dot_general(a, b, (((1,), (0,)), ((), ())), preferred_element_type=F32)


def nt(a, b):
    return lax.dot_general(a, b, (((1,), (1,)), ((), ())), preferred_element_type=F32)


def split(x):
    high = x.astype(BF16).astype(F32)
    return high, x - high


def iota(shape, dim):
    return lax.broadcasted_iota(jnp.int32, shape, dim)


def hot(mask):
    return jnp.where(mask, 1.0, 0.0).astype(F32)


def cat(parts, axis):
    return jnp.concatenate(parts, axis=axis)


def start(sems, *pairs):
    copies = [pltpu.make_async_copy(src, dst, sems.at[i]) for i, (src, dst) in enumerate(pairs)]
    for copy in copies:
        copy.start()
    return copies


def finish(copies):
    for copy in copies:
        copy.wait()


def fetch(sems, *pairs):
    finish(start(sems, *pairs))


def pack_kernel(slabs, pp_in, nm_in, own_in, nod_in, field, kappa, send, place, up, down,
                pp, nm, own, nod, bulk, edges, sems, bulk_sems, out_sems):
    rows = field.shape[2]
    first_layers = (field.shape[1] - 2, 0)
    small = start(sems, (own_in, own), (nod_in, nod), (pp_in, pp), (nm_in, nm))
    loads = []
    for side, z in enumerate(first_layers):
        loads += start(
            bulk_sems.at[side],
            (field.at[:, pl.ds(z, 2)], bulk.at[side, 0:3]),
            (kappa.at[pl.ds(z, 2)], bulk.at[side, 3]),
        )
    finish(small)
    owners = own[...]
    nodes = nod[...].astype(F32)
    depth = pp.shape[1]

    def layer(a, z):
        return cat([a[2 * z : 2 * z + 1], a[2 * z + 1 : 2 * z + 2]], 1)

    ow = [layer(owners, z) for z in range(depth)]
    nd = [layer(nodes, z) for z in range(depth)]
    ids = iota((slabs, 256), 0)
    member = [hot(ow[z] == ids) for z in range(depth)]
    before = hot(iota((256, 256), 0) < iota((256, 256), 1)).astype(BF16)
    counts = nn(cat(member, 0).astype(BF16), before)
    offset = jnp.zeros((slabs, 1), F32)
    slot = iota((4 * CAP, 256), 0)
    rank_row = (slot // 4).astype(F32)
    comp = slot % 4
    words = []
    for z in range(depth):
        seen = counts[slabs * z : slabs * (z + 1)] + offset
        rank = jnp.sum(member[z] * seen, axis=0, keepdims=True)
        offset = offset + jnp.sum(member[z], axis=1, keepdims=True)
        place[z : z + 1] = ow[z].astype(F32) * CAP + rank
        jump = pp[0, z : z + 1] - pp[1, z : z + 1]
        t0, t1, t2 = [jump * nm[c, z : z + 1] for c in range(3)]
        value = jnp.where(comp == 0, t0, jnp.where(comp == 1, t1, jnp.where(comp == 2, t2, nd[z])))
        words.append(jnp.where(rank == rank_row, value, 0.0))
    place[depth:8] = jnp.zeros((8 - depth, 256), F32)
    fill = jnp.zeros((7, 256), F32)
    edges[0] = cat([place[depth - 1 : depth], fill], 0)
    edges[1] = cat([place[0:1], fill], 0)
    finish(loads)
    stores = []
    for side, out in enumerate((up, down)):
        stores += start(
            out_sems.at[side],
            *[(bulk.at[side, c, l], out.at[pl.ds((2 * c + l) * rows, rows)]) for c in range(4) for l in range(2)],
            (edges.at[side], out.at[pl.ds(8 * rows, 8)]),
        )
    high, low = split(cat(words, 1))
    members = cat(member, 1).astype(BF16)
    packed = nt(members, high.astype(BF16)) + nt(members, low.astype(BF16))
    ahead = cat([packed[1:], jnp.zeros((1, 4 * CAP), F32)], 0)
    send[pl.ds(0, slabs, stride=2), :] = packed
    send[pl.ds(1, slabs, stride=2), :] = ahead
    finish(stores)


def stage_kernel(stiffness, conn_in, precond_in, held, conn, precond, table, sems):
    copies = start(sems, (conn_in, conn), (precond_in, precond), (stiffness, held))
    finish(copies[:1])
    connect(corners(conn), table)
    finish(copies[1:])


def corners(conn):
    return [conn[a : a + 1] for a in range(4)]


def connect(nodes, table):
    for a in range(4):
        table[:, a * ELEMS : (a + 1) * ELEMS] = hot(iota((128, ELEMS), 0) == (nodes[a] & 127)).astype(BF16)


def stiff(values, blocks, stiffness, table, spread):
    high, low = split(values)
    parts = []
    for b in range(NBLK):
        lanes = slice(128 * b, 128 * b + 128)
        parts += [high[:, lanes], low[:, lanes]]
    stack = cat(parts, 0).astype(BF16)
    gathered = []
    for a in range(4):
        wide = nn(stack, table[:, a * ELEMS : (a + 1) * ELEMS])
        total = jnp.zeros((8, ELEMS), F32)
        for b in range(NBLK):
            row = wide[16 * b : 16 * b + 8] + wide[16 * b + 8 : 16 * b + 16]
            total = total + jnp.where(blocks[a] == b, row, 0.0)
        gathered.append(total)
    chunk = 256
    pieces = []
    for e in range(0, ELEMS, chunk):
        acc = jnp.zeros((24, chunk), F32)
        for a in range(4):
            for c in range(6):
                acc = acc + stiffness[a * 6 + c, :, e : e + chunk] * gathered[a][c : c + 1, e : e + chunk]
        pieces.append(acc)
    force = cat(pieces, 1)
    for a in range(4):
        part = cat([force[6 * a : 6 * a + 6], jnp.zeros((2, ELEMS), F32)], 0)
        both = cat(split(part), 0)
        for b in range(NBLK):
            spread[16 * b : 16 * b + 16, a * ELEMS : (a + 1) * ELEMS] = jnp.where(
                blocks[a] == b, both, 0.0
            ).astype(BF16)
    summed = nt(spread[...], table[...])
    return cat([summed[16 * b : 16 * b + 8] + summed[16 * b + 8 : 16 * b + 16] for b in range(NBLK)], 1)


def fold(tile):
    both = tile + pltpu.roll(tile, 4, 0)
    return jnp.where(iota(tile.shape, 0) < 3, both, 0.0)


def diagonal(precond, ghost):
    joined = cat([precond[...], ghost[:, :NB]], 1)
    return cat([joined, jnp.zeros((2, EXT), F32)], 0)


def selection(data, r):
    senders = data.shape[1] // 2
    node = data[4 * r + 3 : 4 * r + 4]
    block = jnp.floor(node * (1.0 / 128.0))
    lane = node - 128.0 * block
    late = iota(node.shape, 1) >= senders
    ids = iota((128, node.shape[1]), 0).astype(F32)
    return jnp.where(late, block + 8.0, block), hot(ids == lane).astype(BF16)


def sum_kernel(recv, loads, data_out, low_end, high_end, slots, marks):
    senders = recv.shape[0] // 2
    rows = cat([recv[pl.ds(0, senders, stride=2), :], recv[pl.ds(1, senders, stride=2), :]], 0)
    pad = jnp.zeros((6, 128), F32)
    low_end[...] = cat([recv[2 * senders - 2 : 2 * senders], pad], 0)
    high_end[...] = cat([recv[0:2], pad], 0)
    data = rows.T
    data_out[...] = data
    high, low = split(data)
    width = 2 * senders
    for r in range(CAP):
        lanes = slice(r * width, (r + 1) * width)
        both = cat([high[4 * r : 4 * r + 4], low[4 * r : 4 * r + 4]], 0)
        block, mark = selection(data, r)
        for b in range(0, 10, 2):
            pair = [jnp.where(block == b, both, 0.0), jnp.where(block == b + 1, both, 0.0) if b < 8 else jnp.zeros_like(both)]
            slots[8 * b : 8 * b + 16, lanes] = cat(pair, 0).astype(BF16)
        marks[:, lanes] = mark
    found = nt(slots[...], marks[...])
    loads[...] = cat([fold(found[8 * b : 8 * b + 8]) for b in range(NBLK)], 1)


def load_kernel(mine, other0, other1, other2, precond, ghost, conn, held, table,
                load, first, partial, spill, edge, spread):
    blocks = [n >> 7 for n in corners(conn)]
    total = mine[...] + other0[...] + other1[...] + other2[...]
    root = lax.axis_index("grp") == lax.axis_size("grp") - 1
    loading = total * jnp.where(root, 1.0, 0.0)
    values = diagonal(precond, ghost) * loading
    load[...] = loading
    first[...] = values
    result = stiff(values, blocks, held, table, spread)
    partial[...] = result
    spill[...] = result[:, NODES:]
    edge[...] = result[:, :NB]


def step_kernel(load, first, partial, from_low, from_high, precond, ghost, conn, held, table, second, spill, spread):
    blocks = [n >> 7 for n in corners(conn)]
    scale = diagonal(precond, ghost)
    loading = load[...]
    extra = cat([from_low[...], jnp.zeros((8, NODES - NB), F32), from_high[...]], 1)
    values = first[...] + scale * (loading - (partial[...] + extra))
    result = stiff(values, blocks, held, table, spread)
    own = values + scale * (loading - result)
    taken = scale * result
    second[...] = cat([own[:, :NODES], -taken[:, NODES:]], 1)
    spill[...] = result[:, NODES:]


def look_up(stack, data):
    width = data.shape[1]
    upper = iota((8, width), 0) < 4
    tiles = []
    for t in range(CAP // 2):
        pair = []
        for r in (2 * t, 2 * t + 1):
            block, mark = selection(data, r)
            wide = nn(stack, mark)
            total = jnp.zeros((8, width), F32)
            for b in range(NBLK):
                total = total + jnp.where(block == b, wide[8 * b : 8 * b + 8], 0.0)
            pair.append(total + pltpu.roll(total, 4, 0))
        tiles.append(jnp.where(upper, pair[0], pair[1]))
    return cat(tiles, 0).T


def reply_kernel(mine, other0, other1, other2, data, low_rows, high_rows, send):
    values = mine[...] + other0[...] + other1[...] + other2[...]
    high, low = split(values)
    parts = [p[0:4, 128 * b : 128 * b + 128] for b in range(NBLK) for p in (high, low)]
    stack = cat(parts + [jnp.zeros((8, 128), F32)], 0).astype(BF16)
    count = data.shape[1] // 2
    answer = look_up(stack, data[...])
    gap = jnp.zeros((count - 2, 128), F32)
    ends = cat([low_rows[0:1], high_rows[0:1], gap, low_rows[1:2], high_rows[1:2], gap], 0).T
    outer = look_up(stack, ends)
    for w in range(2):
        part = answer[w * count : (w + 1) * count]
        below = outer[w * count : w * count + 1]
        above = outer[w * count + 1 : w * count + 2]
        send[pl.ds(w, count, stride=6), :] = cat([below, part[: count - 1]], 0)
        send[pl.ds(2 + w, count, stride=6), :] = part
        send[pl.ds(4 + w, count, stride=6), :] = cat([part[1:], above], 0)


def sweep_kernel(field, kappa, place, low, high, out, mid,
                 places, kext, fext, mext, done, edges, sems, out_sems):
    depth = field.shape[1]
    rows, cols = field.shape[2:]
    level = rows // 2
    flat = lax.axis_index("grp") * lax.axis_size("slab") + lax.axis_index("slab")
    last = lax.axis_size("grp") * lax.axis_size("slab") - 1
    pairs = [(kappa, kext.at[2 : depth + 2]), (field, fext.at[:, 2 : depth + 2])]
    for side, (message, start) in enumerate(((low, 0), (high, depth + 2))):
        pairs.append((message.at[8 * rows : 8 * rows + 8], edges.at[side]))
        for l in range(2):
            for c in range(3):
                row = (2 * c + l) * rows
                pairs.append((message.at[row : row + rows], fext.at[c, start + l]))
            row = (6 + l) * rows
            pairs.append((message.at[row : row + rows], kext.at[start + l]))
    fetch(sems, *pairs)
    places[0:1] = edges[0, 0:1]
    places[1 : depth + 1] = place[0:depth]
    places[depth + 1 : depth + 2] = edges[1, 0:1]

    @pl.when(flat == 0)
    def _():
        kext[1] = kext[2]

    @pl.when(flat == last)
    def _():
        kext[depth + 2] = kext[depth + 1]

    row = iota((rows, cols), 0)
    col = iota((rows, cols), 1)

    def weights(l):
        k = kext[l]
        down = k + jnp.where(row == 0, k, pltpu.roll(k, 1, 0))
        up = k + jnp.where(row == rows - 1, k, pltpu.roll(k, rows - 1, 0))
        left = k + jnp.where(col == 0, k, pltpu.roll(k, 1, 1))
        right = k + jnp.where(col == cols - 1, k, pltpu.roll(k, cols - 1, 1))
        back = k + kext[l - 1]
        front = k + kext[l + 1]
        inverse = 1.0 / (down + up + left + right + back + front)
        return (
            jnp.where(row == 0, 0.0, down) * inverse,
            jnp.where(row == rows - 1, 0.0, up) * inverse,
            jnp.where(col == 0, 0.0, left) * inverse,
            jnp.where(col == cols - 1, 0.0, right) * inverse,
            back * inverse,
            front * inverse,
        )

    def blend(w, here, before, after):
        down, up, left, right, back, front = w
        total = down * pltpu.roll(here, 1, 0) + up * pltpu.roll(here, rows - 1, 0)
        total = total + left * pltpu.roll(here, 1, 1) + right * pltpu.roll(here, cols - 1, 1)
        total = total + back * before + front * after
        return jnp.where(row == level, 0.0, total)

    fext[:, :, level : level + 1, :] = jnp.zeros((3, depth + 4, 1, cols), F32)

    def first_sweep(i, carry):
        l = i + 1
        w = weights(l)
        down, up, left, right, back, front = w
        outside = jnp.logical_or(
            jnp.logical_and(flat == 0, i == 0), jnp.logical_and(flat == last, i == depth + 1)
        )
        keep = jnp.where(outside, 0.0, 1.0)
        a, b = level - 1, level - 2
        c, d = level + 1, level + 2
        picked = [
            up[a : a + 1] * keep, back[a : a + 1], front[a : a + 1], left[a : a + 1], right[a : a + 1],
            up[b : b + 1],
            down[c : c + 1] * keep, back[c : c + 1], front[c : c + 1], left[c : c + 1], right[c : c + 1],
            down[d : d + 1],
        ]
        mid[3 * depth + i] = cat(picked + [places[pl.ds(i, 1)], jnp.zeros((3, cols), F32)], 0)
        for comp in range(3):
            mext[comp, i] = blend(w, fext[comp, l], fext[comp, l - 1], fext[comp, l + 1]) * keep
        return carry

    lax.fori_loop(0, depth + 2, first_sweep, 0)

    def second_sweep(z):
        w = weights(z + 2)
        for comp in range(3):
            value = blend(w, mext[comp, z + 1], mext[comp, z], mext[comp, z + 2])
            done[comp, z] = value
            mid[comp * depth + z] = value[LOW : LOW + 16]

    stores = []
    for z in range(depth):
        second_sweep(z)
        stores.append(pltpu.make_async_copy(done.at[:, z], out.at[:, z], out_sems.at[z]))
        stores[z].start()
    for store in stores:
        store.wait()


def finish_kernel(slabs, recv, mid, base, out, rows16, sem):
    depth = rows16.shape[1]
    cols = rows16.shape[3]
    slot = iota((4 * CAP, cols), 0)
    rank_row = (slot // 4).astype(F32)
    ids = iota((slabs, cols), 0).astype(F32)
    views = []
    for j in range(3):
        taken = recv[pl.ds(2 * j + 1, slabs, stride=6), :]
        part = recv[pl.ds(2 * j, slabs, stride=6), :] + cat([jnp.zeros((1, 128), F32), taken[: slabs - 1]], 0)
        views.append(cat(split(part), 0).T.astype(BF16))
    sources = [(j, mid[3 * depth + i, 12:13]) for i, j in enumerate([0] + [1] * depth + [2])]
    motion = []
    for j, where in sources:
        owner = jnp.floor(where * (1.0 / CAP))
        rank = where - CAP * owner
        member = hot(owner == ids).astype(BF16)
        wide = nn(views[j], cat([member, member], 0))
        kept = jnp.where(rank == rank_row, wide, 0.0)
        total = kept[0:8]
        for t in range(1, 4 * CAP // 8):
            total = total + kept[8 * t : 8 * t + 8]
        motion.append(total + pltpu.roll(total, 4, 0))
    f = mid.at[3 * depth : 4 * depth + 2]
    near = [[f[i, 6 * s : 6 * s + 1] * motion[i] for i in range(depth + 2)] for s in range(2)]
    for z in range(depth):
        i = z + 1
        added = []
        for s in range(2):
            o = 6 * s
            d = near[s]
            side = (
                f[i, o + 1 : o + 2] * d[i - 1]
                + f[i, o + 2 : o + 3] * d[i + 1]
                + f[i, o + 3 : o + 4] * pltpu.roll(d[i], 1, 1)
                + f[i, o + 4 : o + 5] * pltpu.roll(d[i], cols - 1, 1)
                + d[i]
            )
            added.append((side, f[i, o + 5 : o + 6] * d[i]))
        (below, below2), (above, above2) = added
        for comp in range(3):
            k = slice(comp, comp + 1)
            change = cat(
                [jnp.zeros((6, cols), F32), below2[k], below[k], motion[i][k], above[k], above2[k],
                 jnp.zeros((5, cols), F32)], 0
            )
            rows16[comp, z] = mid[comp * depth + z] + change
    store = pltpu.make_async_copy(rows16, out.at[:, :, LOW : LOW + 16, :], sem)
    store.start()
    store.wait()


def shape(*dims):
    return jax.ShapeDtypeStruct(dims, F32)


def call(kernel, ins, outs, scratch, mib=8, aliases=None, name=None):
    kinds = {"v": VMEM, "h": HBM, "a": ANY}
    into, out = name.split("_")[1:]
    return pl.pallas_call(
        kernel,
        out_shape=outs,
        in_specs=[kinds[k] for k in into],
        out_specs=[kinds[k] for k in out],
        scratch_shapes=list(scratch),
        input_output_aliases=aliases or {},
        compiler_params=pltpu.CompilerParams(vmem_limit_bytes=mib * MIB),
    )(*ins)


def exchange(rows, per, count):
    flat = rows.reshape(count, 1, per * 128)
    return lax.all_to_all(flat, "slab", 0, 0, tiled=True).reshape(count * per, 128)


def on_device(
    pressure_pair, normals, mesh_disp, kappa, face_owner, face_node, stiffness, shell_conn, precond
):
    groups = lax.axis_size("grp")
    slabs = lax.axis_size("slab")
    count = groups * slabs
    depth, height, across = mesh_disp.shape[1:]
    up = [(i, i + 1) for i in range(count - 1)]
    down = [(b, a) for a, b in up]
    shell = count - slabs
    shell_up = [(shell + i, shell + i + 1) for i in range(slabs - 1)]
    shell_down = [(b, a) for a, b in shell_up]
    dma = pltpu.SemaphoreType.DMA

    ghost = lax.ppermute(precond, AXES, shell_down)
    message = shape(8 * height + 8, across)
    send, place, to_up, to_down = call(
        lambda *refs: pack_kernel(slabs, *refs),
        [pressure_pair, normals, face_owner.reshape(8, 128), face_node.reshape(8, 128), mesh_disp, kappa],
        [shape(2 * slabs, 128), shape(8, across), message, message],
        [
            pltpu.VMEM(pressure_pair.shape, F32),
            pltpu.VMEM(normals.shape, F32),
            pltpu.VMEM((8, 128), jnp.int32),
            pltpu.VMEM((8, 128), jnp.int32),
            pltpu.VMEM((2, 4, 2, height, across), F32),
            pltpu.VMEM((2, 8, across), F32),
            dma((4,)),
            dma((2, 2)),
            dma((2, 9)),
        ],
        mib=63,
        name="pack_hhhhhh_vvhh",
    )
    recv = exchange(send, 2, slabs)
    low = lax.ppermute(to_up, AXES, up)
    high = lax.ppermute(to_down, AXES, down)

    held, conn, diag, table = call(
        stage_kernel,
        [stiffness, shell_conn, precond],
        [
            shape(*stiffness.shape), jax.ShapeDtypeStruct(shell_conn.shape, jnp.int32), shape(*precond.shape),
            jax.ShapeDtypeStruct((128, 4 * ELEMS), BF16),
        ],
        [dma((3,))],
        name="stage_hhh_vvvv",
    )
    spread = pltpu.VMEM((16 * NBLK, 4 * ELEMS), BF16)
    width = 2 * slabs * CAP
    mine, kept, low_end, high_end = call(
        sum_kernel,
        [recv],
        [shape(8, EXT), shape(128, 2 * slabs), shape(8, 128), shape(8, 128)],
        [pltpu.VMEM((80, width), BF16), pltpu.VMEM((128, width), BF16)],
        mib=12,
        name="sum_v_vvvv",
    )
    root = groups - 1
    none = jnp.zeros((8, EXT), F32)
    others = [lax.ppermute(mine, "grp", [(g, root)]) for g in range(root)] + [none] * (4 - groups)
    low_rows = lax.ppermute(low_end, "grp", [(g, g + 1) for g in range(root)])
    high_rows = lax.ppermute(high_end, "grp", [(g + 1, g) for g in range(root)])
    load, first, partial, spill, edge = call(
        load_kernel,
        [mine, *others, diag, ghost, conn, held, table],
        [shape(8, EXT), shape(8, EXT), shape(8, EXT), shape(8, NB), shape(8, NB)],
        [spread],
        mib=16,
        name="load_vvvvvvvvv_vvvvv",
    )
    spill_low = lax.ppermute(spill, AXES, shell_up)
    edge_high = lax.ppermute(edge, AXES, shell_down)
    second, spill = call(
        step_kernel,
        [load, first, partial, spill_low, edge_high, diag, ghost, conn, held, table],
        [shape(8, EXT), shape(8, NB)],
        [spread],
        mib=16,
        name="step_vvvvvvvvvv_vv",
    )
    others = [lax.ppermute(second, "grp", [(root, g)]) for g in range(root)] + [none] * (4 - groups)
    (send,) = call(
        reply_kernel,
        [second, *others, kept, low_rows, high_rows],
        [shape(6 * slabs, 128)],
        [],
        mib=12,
        name="reply_vvvvvvv_v",
    )
    back = exchange(send, 6, slabs)
    spill_low = lax.ppermute(spill, AXES, shell_up)
    shell_disp = second[:6, :NODES].at[:, :NB].add(-(precond[:, :NB] * spill_low[:6]))
    base, mid = call(
        sweep_kernel,
        [mesh_disp, kappa, place, low, high],
        [shape(3, depth, height, across), shape(4 * depth + 2, 16, across)],
        [
            pltpu.VMEM((8, across), F32),
            pltpu.VMEM((depth + 4, height, across), F32),
            pltpu.VMEM((3, depth + 4, height, across), F32),
            pltpu.VMEM((3, depth + 2, height, across), F32),
            pltpu.VMEM((3, depth, height, across), F32),
            pltpu.VMEM((2, 8, across), F32),
            dma((20,)),
            dma((depth,)),
        ],
        mib=16,
        name="sweep_hhvaa_hv",
    )
    (field,) = call(
        lambda *refs: finish_kernel(slabs, *refs),
        [back, mid, base],
        [shape(3, depth, height, across)],
        [pltpu.VMEM((3, depth, 16, across), F32), dma],
        aliases={2: 0},
        name="finish_vvh_h",
    )
    return (field, shell_disp)


def solution(mesh):
    in_specs = (
        P(None, ("grp", "slab"), None),
        P(None, ("grp", "slab"), None),
        P(None, ("grp", "slab"), None, None),
        P(("grp", "slab"), None, None),
        P(("grp", "slab"), None),
        P(("grp", "slab")),
        P(None, None, ("grp", "slab")),
        P(None, ("grp", "slab")),
        P(None, ("grp", "slab")),
    )
    out_specs = (P(None, ("grp", "slab"), None, None), P(None, ("grp", "slab")))
    return jax.shard_map(
        on_device, mesh=mesh, in_specs=in_specs, out_specs=out_specs, check_vma=False
    )
```

```python
import jax
import jax.numpy as jnp
from jax import lax
from jax.experimental import pallas as pl
from jax.experimental.pallas import tpu as pltpu
from jax.sharding import PartitionSpec as P

F32 = jnp.float32
BF16 = jnp.bfloat16
AXES = ("grp", "slab")
CAP = 32
NB = 128
NODES = 1024
EXT = NODES + NB
NBLK = EXT // 128
ELEMS = 1024
LOW = 56
VMEM = pl.BlockSpec(memory_space=pltpu.VMEM)
ANY = pl.BlockSpec(memory_space=pl.ANY)
HBM = pl.BlockSpec(memory_space=pltpu.HBM)
MIB = 1024 * 1024


def nn(a, b):
    return lax.dot_general(a, b, (((1,), (0,)), ((), ())), preferred_element_type=F32)


def nt(a, b):
    return lax.dot_general(a, b, (((1,), (1,)), ((), ())), preferred_element_type=F32)


def split(x):
    high = x.astype(BF16).astype(F32)
    return high, x - high


def iota(shape, dim):
    return lax.broadcasted_iota(jnp.int32, shape, dim)


def hot(mask):
    return jnp.where(mask, 1.0, 0.0).astype(F32)


def cat(parts, axis):
    return jnp.concatenate(parts, axis=axis)


def start(sems, *pairs):
    copies = [pltpu.make_async_copy(src, dst, sems.at[i]) for i, (src, dst) in enumerate(pairs)]
    for copy in copies:
        copy.start()
    return copies


def finish(copies):
    for copy in copies:
        copy.wait()


def pack_kernel(slabs, pp_in, nm_in, own_in, nod_in, field, kappa, send, place, up, down,
                pp, nm, own, nod, bulk, edges, sems, bulk_sems, out_sems):
    rows = field.shape[2]
    first_layers = (field.shape[1] - 2, 0)
    small = start(sems, (own_in, own), (nod_in, nod), (pp_in, pp), (nm_in, nm))
    loads = []
    for side, z in enumerate(first_layers):
        loads += start(
            bulk_sems.at[side],
            (field.at[:, pl.ds(z, 2)], bulk.at[side, 0:3]),
            (kappa.at[pl.ds(z, 2)], bulk.at[side, 3]),
        )
    finish(small)
    owners = own[...]
    nodes = nod[...].astype(F32)
    depth = pp.shape[1]

    def layer(a, z):
        return cat([a[2 * z : 2 * z + 1], a[2 * z + 1 : 2 * z + 2]], 1)

    ow = [layer(owners, z) for z in range(depth)]
    nd = [layer(nodes, z) for z in range(depth)]
    ids = iota((slabs, 256), 0)
    member = [hot(ow[z] == ids) for z in range(depth)]
    before = hot(iota((256, 256), 0) < iota((256, 256), 1)).astype(BF16)
    counts = nn(cat(member, 0).astype(BF16), before)
    offset = jnp.zeros((slabs, 1), F32)
    slot = iota((4 * CAP, 256), 0)
    rank_row = (slot // 4).astype(F32)
    comp = slot % 4
    words = []
    for z in range(depth):
        seen = counts[slabs * z : slabs * (z + 1)] + offset
        rank = jnp.sum(member[z] * seen, axis=0, keepdims=True)
        offset = offset + jnp.sum(member[z], axis=1, keepdims=True)
        place[z : z + 1] = ow[z].astype(F32) * CAP + rank
        jump = pp[0, z : z + 1] - pp[1, z : z + 1]
        t0, t1, t2 = [jump * nm[c, z : z + 1] for c in range(3)]
        value = jnp.where(comp == 0, t0, jnp.where(comp == 1, t1, jnp.where(comp == 2, t2, nd[z])))
        words.append(jnp.where(rank == rank_row, value, 0.0))
    place[depth:8] = jnp.zeros((8 - depth, 256), F32)
    fill = jnp.zeros((7, 256), F32)
    edges[0] = cat([place[depth - 1 : depth], fill], 0)
    edges[1] = cat([place[0:1], fill], 0)
    finish(loads)
    stores = []
    for side, out in enumerate((up, down)):
        stores += start(
            out_sems.at[side],
            *[(bulk.at[side, c, l], out.at[pl.ds((2 * c + l) * rows, rows)]) for c in range(4) for l in range(2)],
            (edges.at[side], out.at[pl.ds(8 * rows, 8)]),
        )
    high, low = split(cat(words, 1))
    members = cat(member, 1).astype(BF16)
    packed = nt(members, high.astype(BF16)) + nt(members, low.astype(BF16))
    ahead = cat([packed[1:], jnp.zeros((1, 4 * CAP), F32)], 0)
    send[pl.ds(0, slabs, stride=2), :] = packed
    send[pl.ds(1, slabs, stride=2), :] = ahead
    finish(stores)


def stage_kernel(stiffness, conn_in, precond_in, held, conn, precond, table, sems):
    copies = start(sems, (conn_in, conn), (precond_in, precond), (stiffness, held))
    finish(copies[:1])
    connect(corners(conn), table)
    finish(copies[1:])


def corners(conn):
    return [conn[a : a + 1] for a in range(4)]


def connect(nodes, table):
    for a in range(4):
        table[:, a * ELEMS : (a + 1) * ELEMS] = hot(iota((128, ELEMS), 0) == (nodes[a] & 127)).astype(BF16)


def stiff(values, blocks, stiffness, table, spread):
    high, low = split(values)
    parts = []
    for b in range(NBLK):
        lanes = slice(128 * b, 128 * b + 128)
        parts += [high[:, lanes], low[:, lanes]]
    stack = cat(parts, 0).astype(BF16)
    gathered = []
    for a in range(4):
        wide = nn(stack, table[:, a * ELEMS : (a + 1) * ELEMS])
        total = jnp.zeros((8, ELEMS), F32)
        for b in range(NBLK):
            row = wide[16 * b : 16 * b + 8] + wide[16 * b + 8 : 16 * b + 16]
            total = total + jnp.where(blocks[a] == b, row, 0.0)
        gathered.append(total)
    chunk = 256
    pieces = []
    for e in range(0, ELEMS, chunk):
        acc = jnp.zeros((24, chunk), F32)
        for a in range(4):
            for c in range(6):
                acc = acc + stiffness[a * 6 + c, :, e : e + chunk] * gathered[a][c : c + 1, e : e + chunk]
        pieces.append(acc)
    force = cat(pieces, 1)
    for a in range(4):
        part = cat([force[6 * a : 6 * a + 6], jnp.zeros((2, ELEMS), F32)], 0)
        both = cat(split(part), 0)
        for b in range(NBLK):
            spread[16 * b : 16 * b + 16, a * ELEMS : (a + 1) * ELEMS] = jnp.where(
                blocks[a] == b, both, 0.0
            ).astype(BF16)
    summed = nt(spread[...], table[...])
    return cat([summed[16 * b : 16 * b + 8] + summed[16 * b + 8 : 16 * b + 16] for b in range(NBLK)], 1)


def fold(tile):
    both = tile + pltpu.roll(tile, 4, 0)
    return jnp.where(iota(tile.shape, 0) < 3, both, 0.0)


def diagonal(precond, ghost):
    joined = cat([precond[...], ghost[:, :NB]], 1)
    return cat([joined, jnp.zeros((2, EXT), F32)], 0)


def selection(data, r):
    senders = data.shape[1] // 2
    node = data[4 * r + 3 : 4 * r + 4]
    block = jnp.floor(node * (1.0 / 128.0))
    lane = node - 128.0 * block
    late = iota(node.shape, 1) >= senders
    ids = iota((128, node.shape[1]), 0).astype(F32)
    return jnp.where(late, block + 8.0, block), hot(ids == lane).astype(BF16)


def sum_kernel(recv, loads, data_out, low_end, high_end, slots, marks):
    senders = recv.shape[0] // 2
    rows = cat([recv[pl.ds(0, senders, stride=2), :], recv[pl.ds(1, senders, stride=2), :]], 0)
    pad = jnp.zeros((6, 128), F32)
    low_end[...] = cat([recv[2 * senders - 2 : 2 * senders], pad], 0)
    high_end[...] = cat([recv[0:2], pad], 0)
    data = rows.T
    data_out[...] = data
    high, low = split(data)
    width = 2 * senders
    for r in range(CAP):
        lanes = slice(r * width, (r + 1) * width)
        both = cat([high[4 * r : 4 * r + 4], low[4 * r : 4 * r + 4]], 0)
        block, mark = selection(data, r)
        for b in range(0, 10, 2):
            pair = [jnp.where(block == b, both, 0.0), jnp.where(block == b + 1, both, 0.0) if b < 8 else jnp.zeros_like(both)]
            slots[8 * b : 8 * b + 16, lanes] = cat(pair, 0).astype(BF16)
        marks[:, lanes] = mark
    found = nt(slots[...], marks[...])
    loads[...] = cat([fold(found[8 * b : 8 * b + 8]) for b in range(NBLK)], 1)


def load_kernel(mine, other0, other1, other2, precond, ghost, conn, held, table,
                load, first, partial, spill, edge, spread):
    blocks = [n >> 7 for n in corners(conn)]
    total = mine[...] + other0[...] + other1[...] + other2[...]
    root = lax.axis_index("grp") == lax.axis_size("grp") - 1
    loading = total * jnp.where(root, 1.0, 0.0)
    values = diagonal(precond, ghost) * loading
    load[...] = loading
    first[...] = values
    result = stiff(values, blocks, held, table, spread)
    partial[...] = result
    spill[...] = result[:, NODES:]
    edge[...] = result[:, :NB]


def step_kernel(load, first, partial, from_low, from_high, precond, ghost, conn, held, table, second, spill, spread):
    blocks = [n >> 7 for n in corners(conn)]
    scale = diagonal(precond, ghost)
    loading = load[...]
    extra = cat([from_low[...], jnp.zeros((8, NODES - NB), F32), from_high[...]], 1)
    values = first[...] + scale * (loading - (partial[...] + extra))
    result = stiff(values, blocks, held, table, spread)
    own = values + scale * (loading - result)
    taken = scale * result
    second[...] = cat([own[:, :NODES], -taken[:, NODES:]], 1)
    spill[...] = result[:, NODES:]


def look_up(stack, data):
    width = data.shape[1]
    upper = iota((8, width), 0) < 4
    tiles = []
    for t in range(CAP // 2):
        pair = []
        for r in (2 * t, 2 * t + 1):
            block, mark = selection(data, r)
            wide = nn(stack, mark)
            total = jnp.zeros((8, width), F32)
            for b in range(NBLK):
                total = total + jnp.where(block == b, wide[8 * b : 8 * b + 8], 0.0)
            pair.append(total + pltpu.roll(total, 4, 0))
        tiles.append(jnp.where(upper, pair[0], pair[1]))
    return cat(tiles, 0).T


def reply_kernel(mine, other0, other1, other2, data, low_rows, high_rows, precond, from_low, swept, send, shell):
    shift = precond[:, :NB] * from_low[0:6]
    shell[...] = cat([mine[0:6, :NB] - shift, mine[0:6, NB:NODES]], 1)
    values = mine[...] + other0[...] + other1[...] + other2[...]
    high, low = split(values)
    parts = [p[0:4, 128 * b : 128 * b + 128] for b in range(NBLK) for p in (high, low)]
    stack = cat(parts + [jnp.zeros((8, 128), F32)], 0).astype(BF16)
    count = data.shape[1] // 2
    answer = look_up(stack, data[...])
    gap = jnp.zeros((count - 2, 128), F32)
    ends = cat([low_rows[0:1], high_rows[0:1], gap, low_rows[1:2], high_rows[1:2], gap], 0).T
    outer = look_up(stack, ends)
    for w in range(2):
        part = answer[w * count : (w + 1) * count]
        below = outer[w * count : w * count + 1]
        above = outer[w * count + 1 : w * count + 2]
        send[pl.ds(w, count, stride=6), :] = cat([below, part[: count - 1]], 0)
        send[pl.ds(2 + w, count, stride=6), :] = part
        send[pl.ds(4 + w, count, stride=6), :] = cat([part[1:], above], 0)


def sweep_kernel(field, kappa, place, low, high, out, mid,
                 places, kext, fext, mext, done, edges, sems, out_sems):
    depth = field.shape[1]
    rows, cols = field.shape[2:]
    level = rows // 2
    flat = lax.axis_index("grp") * lax.axis_size("slab") + lax.axis_index("slab")
    last = lax.axis_size("grp") * lax.axis_size("slab") - 1
    pairs = [(kappa, kext.at[2 : depth + 2]), (field, fext.at[:, 2 : depth + 2])]
    for side, (message, base) in enumerate(((low, 0), (high, depth + 2))):
        pairs.append((message.at[8 * rows : 8 * rows + 8], edges.at[side]))
        for l in range(2):
            for c in range(3):
                row = (2 * c + l) * rows
                pairs.append((message.at[row : row + rows], fext.at[c, base + l]))
            row = (6 + l) * rows
            pairs.append((message.at[row : row + rows], kext.at[base + l]))
    copies = start(sems, *pairs)
    places[1 : depth + 1] = place[0:depth]
    finish(copies[:2])

    row = iota((rows, cols), 0)
    col = iota((rows, cols), 1)

    def weights(l):
        k = kext[l]
        down = k + jnp.where(row == 0, k, pltpu.roll(k, 1, 0))
        up = k + jnp.where(row == rows - 1, k, pltpu.roll(k, rows - 1, 0))
        left = k + jnp.where(col == 0, k, pltpu.roll(k, 1, 1))
        right = k + jnp.where(col == cols - 1, k, pltpu.roll(k, cols - 1, 1))
        back = k + kext[l - 1]
        front = k + kext[l + 1]
        inverse = 1.0 / (down + up + left + right + back + front)
        return (
            jnp.where(row == 0, 0.0, down) * inverse,
            jnp.where(row == rows - 1, 0.0, up) * inverse,
            jnp.where(col == 0, 0.0, left) * inverse,
            jnp.where(col == cols - 1, 0.0, right) * inverse,
            back * inverse,
            front * inverse,
        )

    def blend(w, here, before, after):
        down, up, left, right, back, front = w
        total = down * pltpu.roll(here, 1, 0) + up * pltpu.roll(here, rows - 1, 0)
        total = total + left * pltpu.roll(here, 1, 1) + right * pltpu.roll(here, cols - 1, 1)
        total = total + back * before + front * after
        return jnp.where(row == level, 0.0, total)

    fext[:, 2 : depth + 2, level : level + 1, :] = jnp.zeros((3, depth, 1, cols), F32)

    def first_sweep(i, carry):
        l = i + 1
        w = weights(l)
        down, up, left, right, back, front = w
        outside = jnp.logical_or(
            jnp.logical_and(flat == 0, i == 0), jnp.logical_and(flat == last, i == depth + 1)
        )
        keep = jnp.where(outside, 0.0, 1.0)
        a, b = level - 1, level - 2
        c, d = level + 1, level + 2
        picked = [
            up[a : a + 1] * keep, back[a : a + 1], front[a : a + 1], left[a : a + 1], right[a : a + 1],
            up[b : b + 1],
            down[c : c + 1] * keep, back[c : c + 1], front[c : c + 1], left[c : c + 1], right[c : c + 1],
            down[d : d + 1],
        ]
        mid[3 * depth + i] = cat(picked + [places[pl.ds(i, 1)], jnp.zeros((3, cols), F32)], 0)
        for comp in range(3):
            mext[comp, i] = blend(w, fext[comp, l], fext[comp, l - 1], fext[comp, l + 1]) * keep
        return carry

    lax.fori_loop(2, depth, first_sweep, 0)
    finish(copies[2:])
    places[0:1] = edges[0, 0:1]
    places[depth + 1 : depth + 2] = edges[1, 0:1]
    fext[:, 0:2, level : level + 1, :] = jnp.zeros((3, 2, 1, cols), F32)
    fext[:, depth + 2 : depth + 4, level : level + 1, :] = jnp.zeros((3, 2, 1, cols), F32)

    @pl.when(flat == 0)
    def _():
        kext[1] = kext[2]

    @pl.when(flat == last)
    def _():
        kext[depth + 2] = kext[depth + 1]

    lax.fori_loop(0, 2, first_sweep, 0)
    lax.fori_loop(depth, depth + 2, first_sweep, 0)

    def second_sweep(z):
        w = weights(z + 2)
        for comp in range(3):
            value = blend(w, mext[comp, z + 1], mext[comp, z], mext[comp, z + 2])
            done[comp, z] = value
            mid[comp * depth + z] = value[LOW : LOW + 16]

    stores = []
    for z in range(depth):
        second_sweep(z)
        stores.append(pltpu.make_async_copy(done.at[:, z], out.at[:, z], out_sems.at[z]))
        stores[z].start()
    for store in stores:
        store.wait()


def finish_kernel(slabs, recv, mid, base, out, rows16, sem):
    depth = rows16.shape[1]
    cols = rows16.shape[3]
    slot = iota((4 * CAP, cols), 0)
    rank_row = (slot // 4).astype(F32)
    ids = iota((slabs, cols), 0).astype(F32)
    views = []
    for j in range(3):
        taken = recv[pl.ds(2 * j + 1, slabs, stride=6), :]
        part = recv[pl.ds(2 * j, slabs, stride=6), :] + cat([jnp.zeros((1, 128), F32), taken[: slabs - 1]], 0)
        views.append(cat(split(part), 0).T.astype(BF16))
    sources = [(j, mid[3 * depth + i, 12:13]) for i, j in enumerate([0] + [1] * depth + [2])]
    motion = []
    for j, where in sources:
        owner = jnp.floor(where * (1.0 / CAP))
        rank = where - CAP * owner
        member = hot(owner == ids).astype(BF16)
        wide = nn(views[j], cat([member, member], 0))
        kept = jnp.where(rank == rank_row, wide, 0.0)
        total = kept[0:8]
        for t in range(1, 4 * CAP // 8):
            total = total + kept[8 * t : 8 * t + 8]
        motion.append(total + pltpu.roll(total, 4, 0))
    f = mid.at[3 * depth : 4 * depth + 2]
    near = [[f[i, 6 * s : 6 * s + 1] * motion[i] for i in range(depth + 2)] for s in range(2)]
    for z in range(depth):
        i = z + 1
        added = []
        for s in range(2):
            o = 6 * s
            d = near[s]
            side = (
                f[i, o + 1 : o + 2] * d[i - 1]
                + f[i, o + 2 : o + 3] * d[i + 1]
                + f[i, o + 3 : o + 4] * pltpu.roll(d[i], 1, 1)
                + f[i, o + 4 : o + 5] * pltpu.roll(d[i], cols - 1, 1)
                + d[i]
            )
            added.append((side, f[i, o + 5 : o + 6] * d[i]))
        (below, below2), (above, above2) = added
        for comp in range(3):
            k = slice(comp, comp + 1)
            change = cat(
                [jnp.zeros((6, cols), F32), below2[k], below[k], motion[i][k], above[k], above2[k],
                 jnp.zeros((5, cols), F32)], 0
            )
            rows16[comp, z] = mid[comp * depth + z] + change
    store = pltpu.make_async_copy(rows16, out.at[:, :, LOW : LOW + 16, :], sem)
    store.start()
    store.wait()


def shape(*dims):
    return jax.ShapeDtypeStruct(dims, F32)


def call(kernel, ins, outs, scratch, mib=8, aliases=None, name=None):
    kinds = {"v": VMEM, "h": HBM, "a": ANY}
    into, out = name.split("_")[1:]
    return pl.pallas_call(
        kernel,
        out_shape=outs,
        in_specs=[kinds[k] for k in into],
        out_specs=[kinds[k] for k in out],
        scratch_shapes=list(scratch),
        input_output_aliases=aliases or {},
        compiler_params=pltpu.CompilerParams(vmem_limit_bytes=mib * MIB),
    )(*ins)


def exchange(rows, per, count):
    flat = rows.reshape(count, 1, per * 128)
    return lax.all_to_all(flat, "slab", 0, 0, tiled=True).reshape(count * per, 128)


def on_device(
    pressure_pair, normals, mesh_disp, kappa, face_owner, face_node, stiffness, shell_conn, precond
):
    groups = lax.axis_size("grp")
    slabs = lax.axis_size("slab")
    count = groups * slabs
    depth, height, across = mesh_disp.shape[1:]
    up = [(i, i + 1) for i in range(count - 1)]
    down = [(b, a) for a, b in up]
    shell = count - slabs
    shell_up = [(shell + i, shell + i + 1) for i in range(slabs - 1)]
    shell_down = [(b, a) for a, b in shell_up]
    dma = pltpu.SemaphoreType.DMA

    ghost = lax.ppermute(precond, AXES, shell_down)
    message = shape(8 * height + 8, across)
    send, place, to_up, to_down = call(
        lambda *refs: pack_kernel(slabs, *refs),
        [pressure_pair, normals, face_owner.reshape(8, 128), face_node.reshape(8, 128), mesh_disp, kappa],
        [shape(2 * slabs, 128), shape(8, across), message, message],
        [
            pltpu.VMEM(pressure_pair.shape, F32),
            pltpu.VMEM(normals.shape, F32),
            pltpu.VMEM((8, 128), jnp.int32),
            pltpu.VMEM((8, 128), jnp.int32),
            pltpu.VMEM((2, 4, 2, height, across), F32),
            pltpu.VMEM((2, 8, across), F32),
            dma((4,)),
            dma((2, 2)),
            dma((2, 9)),
        ],
        mib=63,
        name="pack_hhhhhh_vvhh",
    )
    recv = exchange(send, 2, slabs)
    low = lax.ppermute(to_up, AXES, up)
    high = lax.ppermute(to_down, AXES, down)

    held, conn, diag, table = call(
        stage_kernel,
        [stiffness, shell_conn, precond],
        [
            shape(*stiffness.shape), jax.ShapeDtypeStruct(shell_conn.shape, jnp.int32), shape(*precond.shape),
            jax.ShapeDtypeStruct((128, 4 * ELEMS), BF16),
        ],
        [dma((3,))],
        name="stage_hhh_vvvv",
    )
    spread = pltpu.VMEM((16 * NBLK, 4 * ELEMS), BF16)
    width = 2 * slabs * CAP
    mine, kept, low_end, high_end = call(
        sum_kernel,
        [recv],
        [shape(8, EXT), shape(128, 2 * slabs), shape(8, 128), shape(8, 128)],
        [pltpu.VMEM((80, width), BF16), pltpu.VMEM((128, width), BF16)],
        mib=12,
        name="sum_v_vvvv",
    )
    root = groups - 1
    none = jnp.zeros((8, EXT), F32)
    others = []
    for g in range(root):
        others.append(lax.ppermute(mine, "grp", [(g, root)]))
    others += [none] * (4 - groups)
    load, first, partial, spill, edge = call(
        load_kernel,
        [mine, *others, diag, ghost, conn, held, table],
        [shape(8, EXT), shape(8, EXT), shape(8, EXT), shape(8, NB), shape(8, NB)],
        [spread],
        mib=16,
        name="load_vvvvvvvvv_vvvvv",
    )
    spill_low = lax.ppermute(spill, AXES, shell_up)
    edge_high = lax.ppermute(edge, AXES, shell_down)
    second, spill = call(
        step_kernel,
        [load, first, partial, spill_low, edge_high, diag, ghost, conn, held, table],
        [shape(8, EXT), shape(8, NB)],
        [spread],
        mib=16,
        name="step_vvvvvvvvvv_vv",
    )
    others = []
    for g in range(root):
        others.append(lax.ppermute(second, "grp", [(root, g)]))
    others += [none] * (4 - groups)
    spill_low = lax.ppermute(spill, AXES, shell_up)
    low_rows = lax.ppermute(low_end, "grp", [(g, g + 1) for g in range(root)])
    high_rows = lax.ppermute(high_end, "grp", [(g + 1, g) for g in range(root)])
    base, mid = call(
        sweep_kernel,
        [mesh_disp, kappa, place, low, high],
        [shape(3, depth, height, across), shape(4 * depth + 2, 16, across)],
        [
            pltpu.VMEM((8, across), F32),
            pltpu.VMEM((depth + 4, height, across), F32),
            pltpu.VMEM((3, depth + 4, height, across), F32),
            pltpu.VMEM((3, depth + 2, height, across), F32),
            pltpu.VMEM((3, depth, height, across), F32),
            pltpu.VMEM((2, 8, across), F32),
            dma((20,)),
            dma((depth,)),
        ],
        mib=16,
        name="sweep_hhvaa_hv",
    )
    send, shell_disp = call(
        reply_kernel,
        [second, *others, kept, low_rows, high_rows, diag, spill_low, mid],
        [shape(6 * slabs, 128), shape(6, NODES)],
        [],
        mib=12,
        name="reply_vvvvvvvvva_vv",
    )
    back = exchange(send, 6, slabs)
    (field,) = call(
        lambda *refs: finish_kernel(slabs, *refs),
        [back, mid, base],
        [shape(3, depth, height, across)],
        [pltpu.VMEM((3, depth, 16, across), F32), dma],
        aliases={2: 0},
        name="finish_vvh_h",
    )
    return (field, shell_disp)


def solution(mesh):
    in_specs = (
        P(None, ("grp", "slab"), None),
        P(None, ("grp", "slab"), None),
        P(None, ("grp", "slab"), None, None),
        P(("grp", "slab"), None, None),
        P(("grp", "slab"), None),
        P(("grp", "slab")),
        P(None, None, ("grp", "slab")),
        P(None, ("grp", "slab")),
        P(None, ("grp", "slab")),
    )
    out_specs = (P(None, ("grp", "slab"), None, None), P(None, ("grp", "slab")))
    return jax.shard_map(
        on_device, mesh=mesh, in_specs=in_specs, out_specs=out_specs, check_vma=False
    )
```

```python
import jax
import jax.numpy as jnp
from jax import lax
from jax.experimental import pallas as pl
from jax.experimental.pallas import tpu as pltpu
from jax.sharding import PartitionSpec as P

F32 = jnp.float32
BF16 = jnp.bfloat16
AXES = ("grp", "slab")
CAP = 32
NB = 128
NODES = 1024
EXT = NODES + NB
NBLK = EXT // 128
ELEMS = 1024
LOW = 56
VMEM = pl.BlockSpec(memory_space=pltpu.VMEM)
ANY = pl.BlockSpec(memory_space=pl.ANY)
HBM = pl.BlockSpec(memory_space=pltpu.HBM)
MIB = 1024 * 1024


def nn(a, b):
    return lax.dot_general(a, b, (((1,), (0,)), ((), ())), preferred_element_type=F32)


def nt(a, b):
    return lax.dot_general(a, b, (((1,), (1,)), ((), ())), preferred_element_type=F32)


def split(x):
    high = x.astype(BF16).astype(F32)
    return high, x - high


def iota(shape, dim):
    return lax.broadcasted_iota(jnp.int32, shape, dim)


def hot(mask):
    return jnp.where(mask, 1.0, 0.0).astype(F32)


def cat(parts, axis):
    return jnp.concatenate(parts, axis=axis)


def start(sems, *pairs):
    copies = [pltpu.make_async_copy(src, dst, sems.at[i]) for i, (src, dst) in enumerate(pairs)]
    for copy in copies:
        copy.start()
    return copies


def finish(copies):
    for copy in copies:
        copy.wait()


def fetch(sems, *pairs):
    finish(start(sems, *pairs))


def pack_kernel(slabs, pp_in, nm_in, own_in, nod_in, field, kappa, send, place, up, down,
                pp, nm, own, nod, bulk, edges, sems, bulk_sems, out_sems):
    rows = field.shape[2]
    first_layers = (field.shape[1] - 2, 0)
    small = start(sems, (own_in, own), (nod_in, nod), (pp_in, pp), (nm_in, nm))
    loads = []
    for side, z in enumerate(first_layers):
        loads += start(
            bulk_sems.at[side],
            (field.at[:, pl.ds(z, 2)], bulk.at[side, 0:3]),
            (kappa.at[pl.ds(z, 2)], bulk.at[side, 3]),
        )
    finish(small)
    owners = own[...]
    nodes = nod[...].astype(F32)
    depth = pp.shape[1]

    def layer(a, z):
        return cat([a[2 * z : 2 * z + 1], a[2 * z + 1 : 2 * z + 2]], 1)

    ow = [layer(owners, z) for z in range(depth)]
    nd = [layer(nodes, z) for z in range(depth)]
    ids = iota((slabs, 256), 0)
    member = [hot(ow[z] == ids) for z in range(depth)]
    before = hot(iota((256, 256), 0) < iota((256, 256), 1)).astype(BF16)
    counts = nn(cat(member, 0).astype(BF16), before)
    offset = jnp.zeros((slabs, 1), F32)
    slot = iota((4 * CAP, 256), 0)
    rank_row = (slot // 4).astype(F32)
    comp = slot % 4
    words = []
    for z in range(depth):
        seen = counts[slabs * z : slabs * (z + 1)] + offset
        rank = jnp.sum(member[z] * seen, axis=0, keepdims=True)
        offset = offset + jnp.sum(member[z], axis=1, keepdims=True)
        place[z : z + 1] = ow[z].astype(F32) * CAP + rank
        jump = pp[0, z : z + 1] - pp[1, z : z + 1]
        t0, t1, t2 = [jump * nm[c, z : z + 1] for c in range(3)]
        value = jnp.where(comp == 0, t0, jnp.where(comp == 1, t1, jnp.where(comp == 2, t2, nd[z])))
        words.append(jnp.where(rank == rank_row, value, 0.0))
    place[depth:8] = jnp.zeros((8 - depth, 256), F32)
    fill = jnp.zeros((7, 256), F32)
    edges[0] = cat([place[depth - 1 : depth], fill], 0)
    edges[1] = cat([place[0:1], fill], 0)
    finish(loads)
    stores = []
    for side, out in enumerate((up, down)):
        stores += start(
            out_sems.at[side],
            *[(bulk.at[side, c, l], out.at[pl.ds((2 * c + l) * rows, rows)]) for c in range(4) for l in range(2)],
            (edges.at[side], out.at[pl.ds(8 * rows, 8)]),
        )
    high, low = split(cat(words, 1))
    members = cat(member, 1).astype(BF16)
    packed = nt(members, high.astype(BF16)) + nt(members, low.astype(BF16))
    ahead = cat([packed[1:], jnp.zeros((1, 4 * CAP), F32)], 0)
    first = send.shape[0] - 2 * slabs
    send[0:first] = jnp.zeros((first, 128), F32)
    send[pl.ds(first, slabs, stride=2), :] = packed
    send[pl.ds(first + 1, slabs, stride=2), :] = ahead
    finish(stores)


def stage_kernel(stiffness, conn_in, precond_in, held, conn, precond, table, sems):
    copies = start(sems, (conn_in, conn), (precond_in, precond), (stiffness, held))
    finish(copies[:1])
    connect(corners(conn), table)
    finish(copies[1:])


def corners(conn):
    return [conn[a : a + 1] for a in range(4)]


def connect(nodes, table):
    for a in range(4):
        table[:, a * ELEMS : (a + 1) * ELEMS] = hot(iota((128, ELEMS), 0) == (nodes[a] & 127)).astype(BF16)


def stiff(values, blocks, stiffness, table, spread):
    high, low = split(values)
    parts = []
    for b in range(NBLK):
        lanes = slice(128 * b, 128 * b + 128)
        parts += [high[:, lanes], low[:, lanes]]
    stack = cat(parts, 0).astype(BF16)
    gathered = []
    for a in range(4):
        wide = nn(stack, table[:, a * ELEMS : (a + 1) * ELEMS])
        total = jnp.zeros((8, ELEMS), F32)
        for b in range(NBLK):
            row = wide[16 * b : 16 * b + 8] + wide[16 * b + 8 : 16 * b + 16]
            total = total + jnp.where(blocks[a] == b, row, 0.0)
        gathered.append(total)
    chunk = 256
    pieces = []
    for e in range(0, ELEMS, chunk):
        acc = jnp.zeros((24, chunk), F32)
        for a in range(4):
            for c in range(6):
                acc = acc + stiffness[a * 6 + c, :, e : e + chunk] * gathered[a][c : c + 1, e : e + chunk]
        pieces.append(acc)
    force = cat(pieces, 1)
    for a in range(4):
        part = cat([force[6 * a : 6 * a + 6], jnp.zeros((2, ELEMS), F32)], 0)
        both = cat(split(part), 0)
        for b in range(NBLK):
            spread[16 * b : 16 * b + 16, a * ELEMS : (a + 1) * ELEMS] = jnp.where(
                blocks[a] == b, both, 0.0
            ).astype(BF16)
    summed = nt(spread[...], table[...])
    return cat([summed[16 * b : 16 * b + 8] + summed[16 * b + 8 : 16 * b + 16] for b in range(NBLK)], 1)


def fold(tile):
    both = tile + pltpu.roll(tile, 4, 0)
    return jnp.where(iota(tile.shape, 0) < 3, both, 0.0)


def diagonal(precond, ghost):
    joined = cat([precond[...], ghost[:, :NB]], 1)
    return cat([joined, jnp.zeros((2, EXT), F32)], 0)


def load_kernel(recv, precond, ghost, conn, held, table, load, first, partial, spill, edge, kept, spread, slots, marks):
    blocks = [n >> 7 for n in corners(conn)]
    senders = recv.shape[0] // 2
    ids = iota((128, senders), 0).astype(F32)
    for which in (1, 0):
        data = recv[pl.ds(which, senders, stride=2), :].T
        if which == 0:
            kept[...] = data
        high, low = split(data)
        for r in range(CAP):
            lanes = slice(r * senders, (r + 1) * senders)
            node = data[4 * r + 3 : 4 * r + 4]
            both = cat([high[4 * r : 4 * r + 4], low[4 * r : 4 * r + 4]], 0)
            if which == 0:
                block = jnp.floor(node * (1.0 / 128.0))
                node = node - 128.0 * block
                for b in range(0, 8, 2):
                    slots[8 * b : 8 * b + 16, lanes] = cat(
                        [jnp.where(block == b + k, both, 0.0) for k in range(2)], 0
                    ).astype(BF16)
            else:
                slots[0:16, lanes] = cat([both, jnp.zeros_like(both)], 0).astype(BF16)
            marks[:, lanes] = hot(ids == node).astype(BF16)
        if which == 0:
            found = nt(slots[...], marks[...])
            sums = [fold(found[8 * b : 8 * b + 8]) for b in range(8)] + sums
        else:
            sums = [fold(nt(slots[0:16], marks[...])[0:8])]
    loading = cat(sums, 1)
    values = diagonal(precond, ghost) * loading
    load[...] = loading
    first[...] = values
    result = stiff(values, blocks, held, table, spread)
    partial[...] = result
    spill[...] = result[:, NODES:]
    edge[...] = result[:, :NB]


def step_kernel(load, first, partial, from_low, from_high, precond, ghost, conn, held, table, second, spill, spread):
    blocks = [n >> 7 for n in corners(conn)]
    scale = diagonal(precond, ghost)
    loading = load[...]
    extra = cat([from_low[...], jnp.zeros((8, NODES - NB), F32), from_high[...]], 1)
    values = first[...] + scale * (loading - (partial[...] + extra))
    result = stiff(values, blocks, held, table, spread)
    own = values + scale * (loading - result)
    second[...] = own[:, :NODES]
    spill[...] = result[:, NODES:]


def reply_kernel(second, precond, from_low, data, send, shell):
    shift = precond[:, :NB] * from_low[0:6]
    near = second[:, :NB] - cat([shift, jnp.zeros((2, NB), F32)], 0)
    values = cat([near, second[:, NB:]], 1)
    shell[...] = values[0:6]
    high, low = split(values)
    senders = data.shape[1]
    stack = cat(
        [
            part[0:4, 128 * b : 128 * b + 128]
            for b in range(NODES // 128)
            for part in (high, low)
        ],
        0,
    ).astype(BF16)
    data = data[...]
    ids = iota((128, senders), 0).astype(F32)
    upper = iota((8, senders), 0) < 4
    tiles = []
    for t in range(CAP // 2):
        pair = []
        for r in (2 * t, 2 * t + 1):
            node = data[4 * r + 3 : 4 * r + 4]
            block = jnp.floor(node * (1.0 / 128.0))
            wide = nn(stack, hot(ids == node - 128.0 * block).astype(BF16))
            total = jnp.zeros((8, senders), F32)
            for b in range(NODES // 128):
                total = total + jnp.where(block == b, wide[8 * b : 8 * b + 8], 0.0)
            pair.append(total + pltpu.roll(total, 4, 0))
        tiles.append(jnp.where(upper, pair[0], pair[1]))
    answer = cat(tiles, 0).T
    send[pl.ds(0, senders, stride=3), :] = cat([answer[senders - 1 :], answer[: senders - 1]], 0)
    send[pl.ds(1, senders, stride=3), :] = answer
    send[pl.ds(2, senders, stride=3), :] = cat([answer[1:], answer[:1]], 0)


def sweep_kernel(field, kappa, place, low, high, out, mid, factors, places,
                 kext, fext, mext, done, edges, sems, out_sems):
    depth = field.shape[1]
    rows, cols = field.shape[2:]
    level = rows // 2
    flat = lax.axis_index("grp") * lax.axis_size("slab") + lax.axis_index("slab")
    last = lax.axis_size("grp") * lax.axis_size("slab") - 1
    pairs = [(kappa, kext.at[2 : depth + 2]), (field, fext.at[:, 2 : depth + 2])]
    for side, (message, start) in enumerate(((low, 0), (high, depth + 2))):
        pairs.append((message.at[8 * rows : 8 * rows + 8], edges.at[side]))
        for l in range(2):
            for c in range(3):
                row = (2 * c + l) * rows
                pairs.append((message.at[row : row + rows], fext.at[c, start + l]))
            row = (6 + l) * rows
            pairs.append((message.at[row : row + rows], kext.at[start + l]))
    fetch(sems, *pairs)
    places[...] = cat([edges[0, 0:1], place[0:depth], edges[1, 0:1], jnp.zeros((6 - depth, cols), F32)], 0)

    @pl.when(flat == 0)
    def _():
        kext[1] = kext[2]

    @pl.when(flat == last)
    def _():
        kext[depth + 2] = kext[depth + 1]

    row = iota((rows, cols), 0)
    col = iota((rows, cols), 1)

    def weights(l):
        k = kext[l]
        down = k + jnp.where(row == 0, k, pltpu.roll(k, 1, 0))
        up = k + jnp.where(row == rows - 1, k, pltpu.roll(k, rows - 1, 0))
        left = k + jnp.where(col == 0, k, pltpu.roll(k, 1, 1))
        right = k + jnp.where(col == cols - 1, k, pltpu.roll(k, cols - 1, 1))
        back = k + kext[l - 1]
        front = k + kext[l + 1]
        inverse = 1.0 / (down + up + left + right + back + front)
        return (
            jnp.where(row == 0, 0.0, down) * inverse,
            jnp.where(row == rows - 1, 0.0, up) * inverse,
            jnp.where(col == 0, 0.0, left) * inverse,
            jnp.where(col == cols - 1, 0.0, right) * inverse,
            back * inverse,
            front * inverse,
        )

    def blend(w, here, before, after):
        down, up, left, right, back, front = w
        total = down * pltpu.roll(here, 1, 0) + up * pltpu.roll(here, rows - 1, 0)
        total = total + left * pltpu.roll(here, 1, 1) + right * pltpu.roll(here, cols - 1, 1)
        total = total + back * before + front * after
        return jnp.where(row == level, 0.0, total)

    fext[:, :, level : level + 1, :] = jnp.zeros((3, depth + 4, 1, cols), F32)

    def first_sweep(i, carry):
        l = i + 1
        w = weights(l)
        down, up, left, right, back, front = w
        outside = jnp.logical_or(
            jnp.logical_and(flat == 0, i == 0), jnp.logical_and(flat == last, i == depth + 1)
        )
        keep = jnp.where(outside, 0.0, 1.0)
        a, b = level - 1, level - 2
        c, d = level + 1, level + 2
        picked = [
            up[a : a + 1] * keep, back[a : a + 1], front[a : a + 1], left[a : a + 1], right[a : a + 1],
            up[b : b + 1],
            down[c : c + 1] * keep, back[c : c + 1], front[c : c + 1], left[c : c + 1], right[c : c + 1],
            down[d : d + 1],
        ]
        factors[i] = cat(picked + [jnp.zeros((4, cols), F32)], 0)
        for comp in range(3):
            mext[comp, i] = blend(w, fext[comp, l], fext[comp, l - 1], fext[comp, l + 1]) * keep
        return carry

    lax.fori_loop(0, depth + 2, first_sweep, 0)

    def second_sweep(z):
        w = weights(z + 2)
        for comp in range(3):
            value = blend(w, mext[comp, z + 1], mext[comp, z], mext[comp, z + 2])
            done[comp, z] = value
            mid[comp, z] = value[LOW : LOW + 16]

    stores = []
    for z in range(depth):
        second_sweep(z)
        stores.append(pltpu.make_async_copy(done.at[:, z], out.at[:, z], out_sems.at[z]))
        stores[z].start()
    for store in stores:
        store.wait()


def finish_kernel(slabs, recv, places, factors, mid, base, out, rows16, sem):
    depth = mid.shape[1]
    cols = mid.shape[3]
    first = recv.shape[0] - 3 * slabs
    slot = iota((4 * CAP, cols), 0)
    rank_row = (slot // 4).astype(F32)
    ids = iota((slabs, cols), 0).astype(F32)
    views = []
    for j in range(3):
        part = recv[pl.ds(first + j, slabs, stride=3), :]
        views.append(cat(split(part), 0).T.astype(BF16))
    sources = [(j, places[i : i + 1]) for i, j in enumerate([0] + [1] * depth + [2])]
    motion = []
    for j, where in sources:
        owner = jnp.floor(where * (1.0 / CAP))
        rank = where - CAP * owner
        member = hot(owner == ids).astype(BF16)
        wide = nn(views[j], cat([member, member], 0))
        kept = jnp.where(rank == rank_row, wide, 0.0)
        total = kept[0:8]
        for t in range(1, 4 * CAP // 8):
            total = total + kept[8 * t : 8 * t + 8]
        motion.append(total + pltpu.roll(total, 4, 0))
    f = factors
    near = [[f[i, 6 * s : 6 * s + 1] * motion[i] for i in range(depth + 2)] for s in range(2)]
    for z in range(depth):
        i = z + 1
        added = []
        for s in range(2):
            o = 6 * s
            d = near[s]
            side = (
                f[i, o + 1 : o + 2] * d[i - 1]
                + f[i, o + 2 : o + 3] * d[i + 1]
                + f[i, o + 3 : o + 4] * pltpu.roll(d[i], 1, 1)
                + f[i, o + 4 : o + 5] * pltpu.roll(d[i], cols - 1, 1)
                + d[i]
            )
            added.append((side, f[i, o + 5 : o + 6] * d[i]))
        (below, below2), (above, above2) = added
        for comp in range(3):
            k = slice(comp, comp + 1)
            change = cat(
                [jnp.zeros((6, cols), F32), below2[k], below[k], motion[i][k], above[k], above2[k],
                 jnp.zeros((5, cols), F32)], 0
            )
            rows16[comp, z] = mid[comp, z] + change
    store = pltpu.make_async_copy(rows16, out.at[:, :, LOW : LOW + 16, :], sem)
    store.start()
    store.wait()


def shape(*dims):
    return jax.ShapeDtypeStruct(dims, F32)


def call(kernel, ins, outs, scratch, mib=8, aliases=None, name=None):
    kinds = {"v": VMEM, "h": HBM, "a": ANY}
    into, out = name.split("_")[1:]
    return pl.pallas_call(
        kernel,
        out_shape=outs,
        in_specs=[kinds[k] for k in into],
        out_specs=[kinds[k] for k in out],
        scratch_shapes=list(scratch),
        input_output_aliases=aliases or {},
        compiler_params=pltpu.CompilerParams(vmem_limit_bytes=mib * MIB),
    )(*ins)


def exchange(rows, per, count):
    flat = rows.reshape(count, 1, per * 128)
    return lax.all_to_all(flat, AXES, 0, 0, tiled=True).reshape(count * per, 128)


def on_device(
    pressure_pair, normals, mesh_disp, kappa, face_owner, face_node, stiffness, shell_conn, precond
):
    groups = lax.axis_size("grp")
    slabs = lax.axis_size("slab")
    count = groups * slabs
    depth, height, across = mesh_disp.shape[1:]
    up = [(i, i + 1) for i in range(count - 1)]
    down = [(b, a) for a, b in up]
    shell = count - slabs
    shell_up = [(shell + i, shell + i + 1) for i in range(slabs - 1)]
    shell_down = [(b, a) for a, b in shell_up]
    dma = pltpu.SemaphoreType.DMA

    ghost = lax.ppermute(precond, AXES, shell_down)
    message = shape(8 * height + 8, across)
    send, place, to_up, to_down = call(
        lambda *refs: pack_kernel(slabs, *refs),
        [pressure_pair, normals, face_owner.reshape(8, 128), face_node.reshape(8, 128), mesh_disp, kappa],
        [shape(2 * count, 128), shape(8, across), message, message],
        [
            pltpu.VMEM(pressure_pair.shape, F32),
            pltpu.VMEM(normals.shape, F32),
            pltpu.VMEM((8, 128), jnp.int32),
            pltpu.VMEM((8, 128), jnp.int32),
            pltpu.VMEM((2, 4, 2, height, across), F32),
            pltpu.VMEM((2, 8, across), F32),
            dma((4,)),
            dma((2, 2)),
            dma((2, 9)),
        ],
        mib=63,
        name="pack_hhhhhh_vvhh",
    )
    recv = exchange(send, 2, count)
    low = lax.ppermute(to_up, AXES, up)
    high = lax.ppermute(to_down, AXES, down)

    held, conn, diag, table = call(
        stage_kernel,
        [stiffness, shell_conn, precond],
        [
            shape(*stiffness.shape), jax.ShapeDtypeStruct(shell_conn.shape, jnp.int32), shape(*precond.shape),
            jax.ShapeDtypeStruct((128, 4 * ELEMS), BF16),
        ],
        [dma((3,))],
        name="stage_hhh_vvvv",
    )
    spread = pltpu.VMEM((16 * NBLK, 4 * ELEMS), BF16)
    load, first, partial, spill, edge, kept = call(
        load_kernel,
        [recv, diag, ghost, conn, held, table],
        [shape(8, EXT), shape(8, EXT), shape(8, EXT), shape(8, NB), shape(8, NB), shape(128, count)],
        [spread, pltpu.VMEM((64, count * CAP), BF16), pltpu.VMEM((128, count * CAP), BF16)],
        mib=20,
        name="load_vvvvvv_vvvvvv",
    )
    spill_low = lax.ppermute(spill, AXES, shell_up)
    edge_high = lax.ppermute(edge, AXES, shell_down)
    second, spill = call(
        step_kernel,
        [load, first, partial, spill_low, edge_high, diag, ghost, conn, held, table],
        [shape(8, NODES), shape(8, NB)],
        [spread],
        mib=16,
        name="step_vvvvvvvvvv_vv",
    )
    spill_low = lax.ppermute(spill, AXES, shell_up)
    send, shell_disp = call(
        reply_kernel,
        [second, diag, spill_low, kept],
        [shape(3 * count, 128), shape(6, NODES)],
        [],
        mib=12,
        name="reply_vvvv_vv",
    )
    back = exchange(send, 3, count)
    base, mid, factors, places = call(
        sweep_kernel,
        [mesh_disp, kappa, place, low, high],
        [shape(3, depth, height, across), shape(3, depth, 16, across), shape(depth + 2, 16, across), shape(8, across)],
        [
            pltpu.VMEM((depth + 4, height, across), F32),
            pltpu.VMEM((3, depth + 4, height, across), F32),
            pltpu.VMEM((3, depth + 2, height, across), F32),
            pltpu.VMEM((3, depth, height, across), F32),
            pltpu.VMEM((2, 8, across), F32),
            dma((20,)),
            dma((depth,)),
        ],
        mib=16,
        name="sweep_hhvaa_hvvv",
    )
    (field,) = call(
        lambda *refs: finish_kernel(slabs, *refs),
        [back, places, factors, mid, base],
        [shape(3, depth, height, across)],
        [pltpu.VMEM((3, depth, 16, across), F32), dma],
        aliases={4: 0},
        name="finish_vvvvh_h",
    )
    return (field, shell_disp)


def solution(mesh):
    in_specs = (
        P(None, ("grp", "slab"), None),
        P(None, ("grp", "slab"), None),
        P(None, ("grp", "slab"), None, None),
        P(("grp", "slab"), None, None),
        P(("grp", "slab"), None),
        P(("grp", "slab")),
        P(None, None, ("grp", "slab")),
        P(None, ("grp", "slab")),
        P(None, ("grp", "slab")),
    )
    out_specs = (P(None, ("grp", "slab"), None, None), P(None, ("grp", "slab")))
    return jax.shard_map(
        on_device, mesh=mesh, in_specs=in_specs, out_specs=out_specs, check_vma=False
    )
```
